16 devices in a mesh: dp: 2 (over y, z), sp: 8 (over x, core).
Axes of the slice: x: 4, y: 2, z: 1, core: 2. Of those that a mesh axis runs over, the one named last changes fastest.
The devices are a block of a 4x4x8 slice.
Arguments:
- x: bfloat16 [16384, 2048], P(('dp', 'sp')), parts along dimension 0
- gain: bfloat16 [2048], replicated
- wq: bfloat16 [2048, 2048], P('sp')
- wk: bfloat16 [2048, 2048], P('sp')
- wv: bfloat16 [2048, 2048], P('sp')
- wo: bfloat16 [2048, 2048], P('sp')
Outputs:
- output: bfloat16 [16384, 2048], P(('dp', 'sp')), parts along dimension 0
There are 2 independent parts. The reference program is written for one: setup_inputs(seed, part) draws one part's arguments, and reference() takes and returns one part's arrays. A program takes and returns all parts, laid end to end along the dimension named above; an argument that names none is the same for every part.
All inputs are finite; a program needn't handle non-finite values.
Results may differ from the reference program's by a relative error of at most 0.012.
Values are sent between devices in bfloat16 or wider.
A program may use at most 768 MiB of HBM per device.

```python
import jax
import jax.numpy as jnp
from jax import lax

ROWS = 8192
D = 2048
HEADS = 8
KV_HEADS = 8
HEAD = 256
THETA = 10000


def setup_inputs(seed: int = 0, part: int = 0) -> dict:
    kx, kn, kq, kk, kv, ko = jax.random.split(jax.random.key(seed), 6)

    def weights(key, rows, columns):
        return jax.random.normal(key, (rows, columns), jnp.float32) * rows**-0.5

    drawn = {
        "x": jax.random.normal(jax.random.fold_in(kx, part), (ROWS, D), jnp.float32),
        "gain": 1 + 0.1 * jax.random.normal(kn, (D,), jnp.float32),
        "wq": 2 * weights(kq, D, HEADS * HEAD),
        "wk": 2 * weights(kk, D, KV_HEADS * HEAD),
        "wv": 4 * weights(kv, D, KV_HEADS * HEAD),
        "wo": weights(ko, HEADS * HEAD, D),
    }
    return {k: v.astype(jnp.bfloat16) for k, v in drawn.items()}


def normed(x, gain):
    wide = x.astype(jnp.float32)
    scale = lax.rsqrt(jnp.mean(wide * wide, -1, keepdims=True) + 1e-6)
    return (wide * scale * gain.astype(jnp.float32)).astype(jnp.bfloat16)


def turned(t, place, theta):
    half = t.shape[-1] // 2
    angle = place.astype(jnp.float32)[:, None] * theta ** (-jnp.arange(half, dtype=jnp.float32) / half)
    cos, sin = jnp.cos(angle)[:, None], jnp.sin(angle)[:, None]
    a, b = t[..., :half].astype(jnp.float32), t[..., half:].astype(jnp.float32)
    return jnp.concatenate([a * cos - b * sin, b * cos + a * sin], -1).astype(jnp.bfloat16)


def matmul(a, w):
    return jnp.dot(a, w, preferred_element_type=jnp.float32).astype(jnp.bfloat16)


def einsum(form, a, b):
    return jnp.einsum(form, a.astype(jnp.float32), b.astype(jnp.float32))


def attention(q, k, v):
    scores = einsum("tgsd,ugd->gstu", q, k) * q.shape[-1] ** -0.5
    token = jnp.arange(q.shape[0])
    scores = jnp.where(token[:, None] >= token, scores, -jnp.inf)
    weights = jax.nn.softmax(scores, -1).astype(jnp.bfloat16)
    return einsum("gstu,ugd->tgsd", weights, v).astype(jnp.bfloat16)


def reference(x, gain, wq, wk, wv, wo):
    a, place = normed(x, gain), jnp.arange(ROWS)
    q = turned(matmul(a, wq).reshape(ROWS, HEADS, HEAD), place, THETA).reshape(ROWS, KV_HEADS, -1, HEAD)
    k = turned(matmul(a, wk).reshape(ROWS, KV_HEADS, HEAD), place, THETA)
    v = matmul(a, wv).reshape(ROWS, KV_HEADS, HEAD)
    seen = attention(q, k, v).reshape(ROWS, HEADS * HEAD)
    return (x.astype(jnp.float32) + jnp.dot(seen, wo, preferred_element_type=jnp.float32)).astype(jnp.bfloat16)
```

```python
import functools

import jax
import jax.numpy as jnp
from jax import lax
from jax.experimental import pallas as pl
from jax.experimental.pallas import tpu as pltpu
from jax.sharding import PartitionSpec as P

HEAD = 256
THETA = 10000
NEG = -1e30
HIDDEN = 2 * NEG
LOG2E = 1.4426950408889634
MESH = pl.DeviceIdType.MESH
ANY = pl.BlockSpec(memory_space=pl.ANY)
VMEM = pl.BlockSpec(memory_space=pltpu.VMEM)
FINE = 32
ONES = 16
PIECES = 4
STRIP = 512


def _dot(a, b):
    return jnp.dot(a, b, preferred_element_type=jnp.float32)


def _ds(i, size):
    return pl.ds(pl.multiple_of(i * size, size), size)


def _greet(n, me):
    barrier = pltpu.get_barrier_semaphore()
    for t in range(1, n):
        pl.semaphore_signal(barrier, inc=1, device_id={"sp": (me + t) % n}, device_id_type=MESH)
    pl.semaphore_wait(barrier, n - 1)


def _places(n):
    me = lax.axis_index("sp")
    chips = n // 2
    c, k = me // 2, me % 2
    at = lambda dx, dk=0: ((c + dx) % chips) * 2 + (k + dk) % 2
    return me, at


def _project(n, x_ref, gain_ref, wq_ref, wk_ref, wv_ref, trig_ref, q_ref, k_ref, v_ref,
             all_s, w_s, cos_s, sin_s, q_s, k_s, v_s, x_sem, own_sem, w_send, w_recv, arrive, to_core, to_right, to_left, out_sem):
    me, at = _places(n)
    own = x_ref.shape[0]
    depth = wq_ref.shape[0]
    half = HEAD // 2
    size = own // PIECES
    core, right, left, chips = at(0, 1), at(1), at(n // 2 - 1), n // 2
    mats = (wq_ref, wk_ref, wv_ref)

    def w_copy(target, m):
        return pltpu.make_async_remote_copy(
            src_ref=mats[m].at[:, _ds(target, HEAD)], dst_ref=w_s.at[m, _ds(me, depth), :],
            send_sem=w_send.at[target, m], recv_sem=w_recv.at[me, m], device_id={"sp": target}, device_id_type=MESH)

    def w_own(m):
        return pltpu.make_async_copy(mats[m].at[:, _ds(me, HEAD)], w_s.at[m, _ds(me, depth), :], own_sem.at[m])

    def w_wait(source, m):
        pltpu.make_async_remote_copy(
            src_ref=mats[m].at[:, _ds(me, HEAD)], dst_ref=w_s.at[m, _ds(source, depth), :],
            send_sem=w_send.at[source, m], recv_sem=w_recv.at[source, m], device_id={"sp": me}, device_id_type=MESH).wait_recv()

    def piece(target, j, p, send):
        ref = all_s.at[j, _ds(p, size), :]
        return pltpu.make_async_remote_copy(src_ref=ref, dst_ref=ref, send_sem=send.at[j, p], recv_sem=arrive.at[j, p],
                                            device_id={"sp": target}, device_id_type=MESH)

    def outs(j, p):
        place = _ds(j * PIECES + p, size)
        return [pltpu.make_async_copy(q_s.at[:, place], q_ref.at[:, place], out_sem.at[j, p, 0]),
                pltpu.make_async_copy(k_s.at[place, :], k_ref.at[place, :], out_sem.at[j, p, 1]),
                pltpu.make_async_copy(v_s.at[:, place], v_ref.at[:, place], out_sem.at[j, p, 2])]

    def project(j, p):
        rows = _ds(p, size)
        place = _ds(j * PIECES + p, size)
        a = all_s[j, rows, :]
        ct, st = trig_ref[0, pl.ds(FINE + own // FINE + j, 1), :], trig_ref[1, pl.ds(FINE + own // FINE + j, 1), :]
        cf, sf = cos_s[rows, :], sin_s[rows, :]
        cos, sin = ct * cf - st * sf, st * cf + ct * sf

        def turned(t):
            t = t.astype(jnp.bfloat16).astype(jnp.float32)
            lo, hi = t[:, :half], t[:, half:]
            return jnp.concatenate([lo * cos - hi * sin, hi * cos + lo * sin], -1)

        q_s[:, place] = turned(_dot(a, w_s[0])).T.astype(jnp.bfloat16)
        k_s[place, :] = turned(_dot(a, w_s[1])).astype(jnp.bfloat16)
        v_s[0:HEAD, place] = _dot(a, w_s[2]).T.astype(jnp.bfloat16)
        for copy in outs(j, p):
            copy.start()

    _greet(n, me)
    x_copy = pltpu.make_async_copy(x_ref, all_s.at[me], x_sem)
    x_copy.start()
    others = [at(dx, dk) for dx in (2, 1, 3, 0) for dk in (0, 1) if (dx, dk) != (0, 0)]
    for target in others:
        for m in range(3):
            w_copy(target, m).start()
    for m in range(3):
        w_own(m).start()

    def table(m, _):
        cm, sm = trig_ref[0, pl.ds(FINE + m, 1), :], trig_ref[1, pl.ds(FINE + m, 1), :]
        cf, sf = trig_ref[0, 0:FINE, :], trig_ref[1, 0:FINE, :]
        cos_s[_ds(m, FINE), :] = cm * cf - sm * sf
        sin_s[_ds(m, FINE), :] = sm * cf + cm * sf

    x_copy.wait()

    def norm(r, _):
        rows = _ds(r, 32)
        wide = all_s[me, rows, :].astype(jnp.float32)
        scale = lax.rsqrt(jnp.mean(wide * wide, -1, keepdims=True) + 1e-6)
        all_s[me, rows, :] = (wide * scale * gain_ref[...].astype(jnp.float32)).astype(jnp.bfloat16)

    lax.fori_loop(0, own // 32, norm, None)
    lax.fori_loop(0, own // FINE, table, None)
    v_s[HEAD:, :] = jnp.ones((ONES, v_s.shape[1]), jnp.bfloat16)

    for p in range(PIECES):
        piece(right, me, p, to_right).start()
        piece(left, me, PIECES - 1 - p, to_left).start()
        piece(core, me, p, to_core).start()

    for m in range(3):
        w_own(m).wait()
    for source in others:
        for m in range(3):
            w_wait(source, m)

    def near(t, _):
        other = t // PIECES
        j, p = me + other * (core - me), t % PIECES

        @pl.when(other == 1)
        def _():
            piece(me, j, p, to_core).wait_recv()

        project(j, p)

    lax.fori_loop(0, 2 * PIECES, near, None)

    def arrived(j_left, p_left, j_right, p_right, forward):
        piece(me, j_left, p_left, to_core).wait_recv()
        piece(core, j_left, p_left, to_core).start()
        if forward is not None:
            @pl.when(forward)
            def _():
                piece(right, j_left, p_left, to_right).start()
        piece(me, j_right, p_right, to_core).wait_recv()
        piece(core, j_right, p_right, to_core).start()
        if forward is not None:
            @pl.when(forward)
            def _():
                piece(left, j_right, p_right, to_left).start()

    def four(j_left, p_left, j_right, p_right):
        def one(t, _):
            side, other = t % 2, t // 2
            j = j_left + side * (j_right - j_left) + other * (core - me)
            p = p_left + side * (p_right - p_left)

            @pl.when(other == 1)
            def _():
                piece(me, j, p, to_core).wait_recv()

            project(j, p)

        lax.fori_loop(0, 4, one, None)

    def next_chips(p, _):
        arrived(left, p, right, PIECES - 1 - p, p < PIECES // 2)
        four(left, p, right, PIECES - 1 - p)

    lax.fori_loop(0, PIECES, next_chips, None)
    far = at(chips // 2)

    def far_chip(p, _):
        arrived(far, p, far, PIECES - 1 - p, None)
        four(far, p, far, PIECES - 1 - p)

    lax.fori_loop(0, PIECES // 2, far_chip, None)

    for target in others:
        for m in range(3):
            w_copy(target, m).wait_send()

    def sent(p, _):
        piece(right, me, p, to_right).wait_send()
        piece(left, me, p, to_left).wait_send()
        for j in (me, left, right, far):
            piece(core, j, p, to_core).wait_send()
        for j in range(n):
            for copy in outs(j, p):
                copy.wait()

    lax.fori_loop(0, PIECES, sent, None)

    def passed(p, _):
        piece(right, left, p, to_right).wait_send()
        piece(left, right, PIECES - 1 - p, to_left).wait_send()

    lax.fori_loop(0, PIECES // 2, passed, None)


def _attend(n, q_ref, k_ref, v_ref, x_ref, wo_ref, y_ref,
            q_s, k_s, v_s, wo_s, o_s, stage, x_s, top_s, mix_s, in_sem, own_sem, y_sem, arrive, to_core, to_right, to_left, o_send, o_recv):
    me, at = _places(n)
    own = x_ref.shape[0]
    depth = wo_ref.shape[0]
    hd = depth // 2
    core, right, left, far = at(0, 1), at(1), at(n // 2 - 1), at(n // 4)
    e = HEAD**-0.5 * LOG2E

    def turn(s):
        u, w = s // 2, s % 2
        m = (1 - w) * (n // 2 + u) + w * (n // 2 - 1 - u)
        d, bit = 0, 1
        while bit < n:
            a, b = (me // bit) % 2, (m // bit) % 2
            d = d + bit * (a + b - 2 * a * b)
            bit *= 2
        return d

    def part(target, j, h, send):
        ref = wo_s.at[_ds(j * 2 + h, hd), :]
        return pltpu.make_async_remote_copy(src_ref=ref, dst_ref=ref, send_sem=send.at[j, h], recv_sem=arrive.at[j, h],
                                            device_id={"sp": target}, device_id_type=MESH)

    def part_own(target, h, send):
        return pltpu.make_async_remote_copy(src_ref=wo_ref.at[h * hd : (h + 1) * hd, :], dst_ref=wo_s.at[_ds(me * 2 + h, hd), :],
                                            send_sem=send.at[me, h], recv_sem=arrive.at[me, h], device_id={"sp": target}, device_id_type=MESH)

    def result(s):
        d = turn(s)
        return pltpu.make_async_remote_copy(src_ref=stage.at[s], dst_ref=o_s.at[:, _ds(me, HEAD)], send_sem=o_send.at[s],
                                            recv_sem=o_recv.at[me], device_id={"sp": d}, device_id_type=MESH)

    loads = [pltpu.make_async_copy(k_ref, k_s, in_sem.at[0]), pltpu.make_async_copy(q_ref, q_s, in_sem.at[1]),
             pltpu.make_async_copy(v_ref, v_s, in_sem.at[2])]
    for load in loads:
        load.start()
    wo_own = pltpu.make_async_copy(wo_ref, wo_s.at[_ds(me, depth), :], own_sem.at[0])
    x_load = pltpu.make_async_copy(x_ref, x_s, own_sem.at[1])
    _greet(n, me)
    for h in range(2):
        part_own(right, h, to_right).start()
        part_own(left, 1 - h, to_left).start()
        part_own(core, h, to_core).start()
    wo_own.start()
    x_load.start()
    for load in loads:
        load.wait()

    def weigh(key, count, d, at_q, masked):
        cols = slice(at_q, at_q + STRIP)
        s = _dot(k_s[pl.ds(pl.multiple_of(key, STRIP), count), :], q_s[:, pl.ds(pl.multiple_of(d * own + at_q, STRIP), STRIP)])
        if masked:
            ok = lax.broadcasted_iota(jnp.int32, s.shape, 1) >= lax.broadcasted_iota(jnp.int32, s.shape, 0)
            s = jnp.where(ok, s, HIDDEN)
        return s

    def soften(s, cols):
        old = top_s[:, cols]
        top = jnp.maximum(old, s.max(axis=0, keepdims=True))
        top_s[:, cols] = top
        return jnp.exp2((s - top) * e).astype(jnp.bfloat16), jnp.exp2((old - top) * e)

    def add(key, count, p, keep, cols):
        mix_s[:, cols] = mix_s[:, cols] * keep + _dot(v_s[:, pl.ds(pl.multiple_of(key, STRIP), count)], p)

    def blocks(items, d):
        scores = [weigh(key, count, d, at_q, masked) for key, count, at_q, masked in items]
        soft = [soften(s, slice(i[2], i[2] + STRIP)) for s, i in zip(scores, items)]
        for (p, keep), (key, count, at_q, _) in zip(soft, items):
            add(key, count, p, keep, slice(at_q, at_q + STRIP))

    strips = range(0, own, STRIP)

    def step(s, _):
        d = turn(s)
        top_s[...] = jnp.full_like(top_s, NEG)
        mix_s[...] = jnp.zeros_like(mix_s)
        for b in strips:
            blocks([(d * own + b, STRIP, at_q, at_q == b) for at_q in strips if at_q >= b], d)

        @pl.when(s > 0)
        def _():
            result(s - 1).start()

        @pl.when(s == 2)
        def _():
            for j, h, target, send in ((left, 0, right, to_right), (right, 1, left, to_left)):
                part(me, j, h, to_core).wait_recv()
                part(target, j, h, send).start()
                part(core, j, h, to_core).start()

        @pl.when(s == 4)
        def _():
            for j, h in ((left, 1), (right, 0)):
                part(me, j, h, to_core).wait_recv()
                part(core, j, h, to_core).start()

        @pl.when(s == 6)
        def _():
            for h in range(2):
                part(me, far, h, to_core).wait_recv()
                part(core, far, h, to_core).start()

        def earlier(b, _):
            blocks([(b * own, own, at_q, False) for at_q in strips], d)

        lax.fori_loop(0, d, earlier, None)
        out = (mix_s[0:HEAD, :] * (1 / mix_s[HEAD : HEAD + 1, :])).T.astype(jnp.bfloat16)

        @pl.when(s < n - 1)
        def _():
            stage[s] = out

        @pl.when(s == n - 1)
        def _():
            o_s[:, _ds(me, HEAD)] = out

    lax.fori_loop(0, n, step, None)

    for h in range(2):
        for j in (core, at(1, 1), at(n // 2 - 1, 1), at(n // 4, 1)):
            part(me, j, h, to_core).wait_recv()
    wo_own.wait()
    x_load.wait()
    for t in range(1, n):
        j = (me + t) % n
        pltpu.make_async_remote_copy(src_ref=stage.at[0], dst_ref=o_s.at[:, _ds(j, HEAD)], send_sem=o_send.at[0],
                                     recv_sem=o_recv.at[j], device_id={"sp": me}, device_id_type=MESH).wait_recv()
    wide, tall = 256, 512

    def y_copy(t):
        return pltpu.make_async_copy(x_s.at[:, _ds(t, wide)], y_ref.at[:, _ds(t, wide)], y_sem.at[t])

    def finish(t, _):
        for r in range(0, own, tall):
            x_s[r : r + tall, _ds(t, wide)] = (x_s[r : r + tall, _ds(t, wide)].astype(jnp.float32)
                                               + _dot(o_s[r : r + tall, :], wo_s[:, _ds(t, wide)])).astype(jnp.bfloat16)
        y_copy(t).start()

    lax.fori_loop(0, y_ref.shape[1] // wide, finish, None)
    for h in range(2):
        part_own(right, h, to_right).wait_send()
        part_own(left, h, to_left).wait_send()
        part_own(core, h, to_core).wait_send()
        for j in (left, right, far):
            part(core, j, h, to_core).wait_send()
    part(right, left, 0, to_right).wait_send()
    part(left, right, 1, to_left).wait_send()
    for s in range(n - 1):
        result(s).wait_send()
    for t in range(y_ref.shape[1] // wide):
        y_copy(t).wait()


def solution(mesh):
    n = mesh.shape["sp"]

    def step(x, gain, wq, wk, wv, wo):
        own, d = x.shape
        tokens, half, low = own * n, HEAD // 2, jnp.bfloat16
        places = jnp.concatenate([jnp.arange(FINE), FINE * jnp.arange(own // FINE), own * jnp.arange(n)]).astype(jnp.float32)
        angle = places[:, None] * THETA ** (-jnp.arange(half, dtype=jnp.float32) / half)
        trig = jnp.stack([jnp.cos(angle), jnp.sin(angle)])
        dma = pltpu.SemaphoreType.DMA
        q, k, v = pl.pallas_call(
            functools.partial(_project, n),
            name="project",
            out_shape=[jax.ShapeDtypeStruct((HEAD, tokens), low), jax.ShapeDtypeStruct((tokens, HEAD), low),
                       jax.ShapeDtypeStruct((HEAD + ONES, tokens), low)],
            in_specs=[ANY, VMEM, ANY, ANY, ANY, VMEM],
            out_specs=[ANY] * 3,
            scratch_shapes=[
                pltpu.VMEM((n, own, d), low), pltpu.VMEM((3, d, HEAD), low), pltpu.VMEM((own, half), jnp.float32), pltpu.VMEM((own, half), jnp.float32),
                pltpu.VMEM((HEAD, tokens), low), pltpu.VMEM((tokens, HEAD), low), pltpu.VMEM((HEAD + ONES, tokens), low),
                dma, dma((3,)), dma((n, 3)), dma((n, 3)), dma((n, PIECES)), dma((n, PIECES)), dma((n, PIECES)), dma((n, PIECES)), dma((n, PIECES, 3)),
            ],
            compiler_params=pltpu.CompilerParams(collective_id=0, has_side_effects=True, vmem_limit_bytes=63 * 2**20),
        )(x, gain.reshape(1, d), wq, wk, wv, trig)
        return pl.pallas_call(
            functools.partial(_attend, n),
            name="attend",
            out_shape=jax.ShapeDtypeStruct((own, d), low),
            in_specs=[ANY] * 5,
            out_specs=ANY,
            scratch_shapes=[
                pltpu.VMEM((HEAD, tokens), low), pltpu.VMEM((tokens, HEAD), low), pltpu.VMEM((HEAD + ONES, tokens), low),
                pltpu.VMEM((d, d), low), pltpu.VMEM((own, d), low), pltpu.VMEM((n - 1, own, HEAD), low), pltpu.VMEM((own, d), low),
                pltpu.VMEM((1, own), jnp.float32), pltpu.VMEM((HEAD + ONES, own), jnp.float32),
                dma((3,)), dma((2,)), dma((d // 256,)), dma((n, 2)), dma((n, 2)), dma((n, 2)), dma((n, 2)), dma((n,)), dma((n,)),
            ],
            compiler_params=pltpu.CompilerParams(collective_id=1, has_side_effects=True, vmem_limit_bytes=63 * 2**20),
        )(q, k, v, x, wo)

    tokens, whole = P(("dp", "sp"), None), P("sp", None)
    return jax.shard_map(step, mesh=mesh, in_specs=(tokens, P(None), whole, whole, whole, whole), out_specs=tokens, check_vma=False)
```

```python
import functools

import jax
import jax.numpy as jnp
from jax import lax
from jax.experimental import pallas as pl
from jax.experimental.pallas import tpu as pltpu
from jax.sharding import PartitionSpec as P

HEAD = 256
THETA = 10000
NEG = -1e30
HIDDEN = 2 * NEG
LOG2E = 1.4426950408889634
MESH = pl.DeviceIdType.MESH
ANY = pl.BlockSpec(memory_space=pl.ANY)
VMEM = pl.BlockSpec(memory_space=pltpu.VMEM)
FINE = 32
ONES = 8
PIECES = 4
STRIP = 512


def _dot(a, b):
    return jnp.dot(a, b, preferred_element_type=jnp.float32)


def _ds(i, size):
    return pl.ds(pl.multiple_of(i * size, size), size)


def _greet(n, me):
    barrier = pltpu.get_barrier_semaphore()
    for t in range(1, n):
        pl.semaphore_signal(barrier, inc=1, device_id={"sp": (me + t) % n}, device_id_type=MESH)
    pl.semaphore_wait(barrier, n - 1)


def _places(n):
    me = lax.axis_index("sp")
    chips = n // 2
    c, k = me // 2, me % 2
    at = lambda dx, dk=0: ((c + dx) % chips) * 2 + (k + dk) % 2
    return me, at


def _xor(n, a, b):
    out, bit = 0, 1
    while bit < n:
        x, y = (a // bit) % 2, (b // bit) % 2
        out = out + bit * (x + y - 2 * x * y)
        bit *= 2
    return out


def _mask(n, s):
    u, w = s // 2, s % 2
    return (1 - w) * (n // 2 + u) + w * (n // 2 - 1 - u)


def _step(n, m):
    far = m // (n // 2)
    return far * 2 * (m - n // 2) + (1 - far) * (2 * (n // 2 - 1 - m) + 1)


def _layer(n, x_ref, gain_ref, wq_ref, wk_ref, wv_ref, wo_ref, trig_ref, y_ref,
           all_s, w_s, cos_s, sin_s, q_s, k_s, v_s, top_s, mix_s,
           x_sem, own_sem, w_send, w_recv, arrive, to_core, to_right, to_left, ready,
           wo_arrive, wo_core, wo_right, wo_left, o_send, o_recv, y_sem):
    me, at = _places(n)
    own, width = x_ref.shape
    depth = wq_ref.shape[0]
    half = HEAD // 2
    size = own // PIECES
    chips = n // 2
    chip = me // 2
    core, right, left, far = at(0, 1), at(1), at(chips - 1), at(chips // 2)
    mats = (wq_ref, wk_ref, wv_ref)
    others = [at(dx, dk) for dx in (2, 1, 3, 0) for dk in (0, 1) if (dx, dk) != (0, 0)]

    def w_copy(target, m):
        return pltpu.make_async_remote_copy(
            src_ref=mats[m].at[:, _ds(target, HEAD)], dst_ref=w_s.at[m, _ds(me, depth), :],
            send_sem=w_send.at[target, m], recv_sem=w_recv.at[me, m], device_id={"sp": target}, device_id_type=MESH)

    def w_own(m):
        return pltpu.make_async_copy(mats[m].at[:, _ds(me, HEAD)], w_s.at[m, _ds(me, depth), :], own_sem.at[m])

    def w_wait(source, m):
        pltpu.make_async_remote_copy(
            src_ref=mats[m].at[:, _ds(me, HEAD)], dst_ref=w_s.at[m, _ds(source, depth), :],
            send_sem=w_send.at[source, m], recv_sem=w_recv.at[source, m], device_id={"sp": me}, device_id_type=MESH).wait_recv()

    def piece(target, j, p, send):
        ref = all_s.at[j, _ds(p, size), :]
        return pltpu.make_async_remote_copy(src_ref=ref, dst_ref=ref, send_sem=send.at[j, p], recv_sem=arrive.at[j, p],
                                            device_id={"sp": target}, device_id_type=MESH)

    hd = depth // 2
    per = own // depth

    def wo_at(d, j, h):
        s = _step(n, _xor(n, d, j))
        return all_s.at[d // 2 * 2 + s // per, _ds((s % per) * 2 + h, hd), :]

    def wo_part(target, j, h, send):
        return pltpu.make_async_remote_copy(src_ref=wo_at(me, j, h), dst_ref=wo_at(target, j, h), send_sem=send.at[j, h],
                                            recv_sem=wo_arrive.at[j, h], device_id={"sp": target}, device_id_type=MESH)

    def wo_first(target, h, send):
        return pltpu.make_async_remote_copy(src_ref=wo_ref.at[h * hd : (h + 1) * hd, :], dst_ref=wo_at(target, me, h),
                                            send_sem=send.at[me, h], recv_sem=wo_arrive.at[me, h], device_id={"sp": target}, device_id_type=MESH)

    def wo_own(h):
        return pltpu.make_async_copy(wo_ref.at[h * hd : (h + 1) * hd, :], wo_at(me, me, h), own_sem.at[h])

    def o_at(d):
        return (d // 2 + chips - 1) % chips * 2 + (d + 1) % 2

    stage = at(1, 1)

    def result(s):
        d = _xor(n, me, _mask(n, s))
        return pltpu.make_async_remote_copy(src_ref=all_s.at[stage, :, _ds(s, HEAD)], dst_ref=all_s.at[o_at(d), :, _ds(s, HEAD)],
                                            send_sem=o_send.at[s], recv_sem=o_recv.at[s], device_id={"sp": d}, device_id_type=MESH)

    def project(j, p):
        rows = _ds(p, size)
        place = _ds(j * PIECES + p, size)
        a = all_s[j, rows, :]
        ct, st = trig_ref[0, pl.ds(FINE + own // FINE + j, 1), :], trig_ref[1, pl.ds(FINE + own // FINE + j, 1), :]
        cf, sf = cos_s[rows, :], sin_s[rows, :]
        cos, sin = ct * cf - st * sf, st * cf + ct * sf

        def turned(t):
            t = t.astype(jnp.bfloat16).astype(jnp.float32)
            lo, hi = t[:, :half], t[:, half:]
            return jnp.concatenate([lo * cos - hi * sin, hi * cos + lo * sin], -1)

        q_s[:, place] = turned(_dot(a, w_s[0])).T.astype(jnp.bfloat16)
        k_s[place, :] = turned(_dot(a, w_s[1])).astype(jnp.bfloat16)
        v_s[0:HEAD, place] = _dot(a, w_s[2]).T.astype(jnp.bfloat16)

    e = HEAD**-0.5 * LOG2E
    strips = range(0, own, STRIP)

    def strip(d, at_q):
        return pl.ds(pl.multiple_of(d * own + at_q, STRIP), STRIP)

    def scores(b, count, d, at_q):
        return _dot(k_s[pl.ds(pl.multiple_of(b * own, own), count), :], q_s[:, strip(d, at_q)])

    def values(b, count):
        return v_s[:, pl.ds(pl.multiple_of(b * own, own), count)]

    def itself(d):
        found = []
        for at_q in strips:
            s = scores(d, at_q + STRIP, d, at_q)
            ok = lax.broadcasted_iota(jnp.int32, s.shape, 1) + at_q >= lax.broadcasted_iota(jnp.int32, s.shape, 0)
            found.append(jnp.where(ok, s, HIDDEN))
        weights = []
        for at_q, s in zip(strips, found):
            top = s.max(axis=0, keepdims=True)
            top_s[:, strip(d, at_q)] = top
            weights.append(jnp.exp2((s - top) * e).astype(jnp.bfloat16))
        for at_q, p in zip(strips, weights):
            mix_s[:, strip(d, at_q)] = _dot(values(d, at_q + STRIP), p)

    def earlier(b, d):
        found = [scores(b, own, d, at_q) for at_q in strips]
        weights = []
        for at_q, s in zip(strips, found):
            old = top_s[:, strip(d, at_q)]
            top = jnp.maximum(old, s.max(axis=0, keepdims=True))
            top_s[:, strip(d, at_q)] = top
            weights.append((jnp.exp2((s - top) * e).astype(jnp.bfloat16), jnp.exp2((old - top) * e)))
        for at_q, (p, keep) in zip(strips, weights):
            mix_s[:, strip(d, at_q)] = mix_s[:, strip(d, at_q)] * keep + _dot(values(b, own), p)

    def attend(d, fresh, need):
        if fresh is True:
            itself(d)
        else:
            pl.when(fresh)(lambda: itself(d))

        def one(b, _):
            pl.when(need(b))(lambda: earlier(b, d))

        lax.fori_loop(0, d, one, None)

    _greet(n, me)
    x_copy = pltpu.make_async_copy(x_ref, all_s.at[me], x_sem)
    x_copy.start()
    for target in others:
        for m in range(3):
            w_copy(target, m).start()
    for m in range(3):
        w_own(m).start()
    x_copy.wait()

    def norm(r, _):
        rows = _ds(r, 32)
        wide = all_s[me, rows, :].astype(jnp.float32)
        scale = lax.rsqrt(jnp.mean(wide * wide, -1, keepdims=True) + 1e-6)
        all_s[me, rows, :] = (wide * scale * gain_ref[...].astype(jnp.float32)).astype(jnp.bfloat16)

    lax.fori_loop(0, own // 32, norm, None)

    def table(m, _):
        cm, sm = trig_ref[0, pl.ds(FINE + m, 1), :], trig_ref[1, pl.ds(FINE + m, 1), :]
        cf, sf = trig_ref[0, 0:FINE, :], trig_ref[1, 0:FINE, :]
        cos_s[_ds(m, FINE), :] = cm * cf - sm * sf
        sin_s[_ds(m, FINE), :] = sm * cf + cm * sf

    lax.fori_loop(0, own // FINE, table, None)
    v_s[HEAD:, :] = jnp.ones((ONES, v_s.shape[1]), jnp.bfloat16)
    for p in range(PIECES):
        piece(right, me, p, to_right).start()
        piece(left, me, PIECES - 1 - p, to_left).start()
        piece(core, me, p, to_core).start()
    for m in range(3):
        w_own(m).wait()
    for source in others:
        for m in range(3):
            w_wait(source, m)

    def near(t, _):
        other = t // PIECES
        j, p = me + other * (core - me), t % PIECES
        pl.when(other == 1)(lambda: piece(me, j, p, to_core).wait_recv())
        project(j, p)

    lax.fori_loop(0, 2 * PIECES, near, None)
    lax.fori_loop(0, 2, lambda i, _: attend(chip * 2 + i, True, lambda b: b // 2 == chip), None)

    def arrived(j_left, p_left, j_right, p_right, forward):
        for j, p, target, send in ((j_left, p_left, right, to_right), (j_right, p_right, left, to_left)):
            piece(me, j, p, to_core).wait_recv()
            piece(core, j, p, to_core).start()
            if forward is not None:
                pl.when(forward)(lambda: piece(target, j, p, send).start())

    def four(j_left, p_left, j_right, p_right):
        def one(t, _):
            side, other = t % 2, t // 2
            j = j_left + side * (j_right - j_left) + other * (core - me)
            p = p_left + side * (p_right - p_left)
            pl.when(other == 1)(lambda: piece(me, j, p, to_core).wait_recv())
            project(j, p)

        lax.fori_loop(0, 4, one, None)

    def next_chips(p, _):
        arrived(left, p, right, PIECES - 1 - p, p < PIECES // 2)
        four(left, p, right, PIECES - 1 - p)

    lax.fori_loop(0, PIECES, next_chips, None)

    def sent(p, _):
        piece(right, me, p, to_right).wait_send()
        piece(left, me, p, to_left).wait_send()
        for j in (me, left, right):
            piece(core, j, p, to_core).wait_send()

    lax.fori_loop(0, PIECES, sent, None)
    for target in others:
        pl.semaphore_signal(ready, inc=1, device_id={"sp": target}, device_id_type=MESH)
    pl.semaphore_wait(ready, n - 1)
    for h in range(2):
        wo_first(right, h, wo_right).start()
        wo_first(left, 1 - h, wo_left).start()
        wo_first(core, h, wo_core).start()
        wo_own(h).start()

    def middle(i, _):
        t = i // 2
        d = (chip + chips - 1 + t) % chips * 2 + i % 2
        attend(d, t != 1, lambda b: (b // 2 != far // 2) & ((t != 1) | (b // 2 != chip)))

    lax.fori_loop(0, 6, middle, None)

    def far_chip(p, _):
        arrived(far, p, far, PIECES - 1 - p, None)
        four(far, p, far, PIECES - 1 - p)

    lax.fori_loop(0, PIECES // 2, far_chip, None)
    lax.fori_loop(0, PIECES, lambda p, _: piece(core, far, p, to_core).wait_send(), None)

    def passed(p, _):
        piece(right, left, p, to_right).wait_send()
        piece(left, right, PIECES - 1 - p, to_left).wait_send()

    lax.fori_loop(0, PIECES // 2, passed, None)
    x_again = pltpu.make_async_copy(x_ref, all_s.at[left], x_sem)
    x_again.start()

    def last(s, _):
        d = _xor(n, me, _mask(n, s))
        in_far = d // 2 == far // 2
        attend(d, in_far, lambda b: in_far | (b // 2 == far // 2))

        @pl.when(s == 2)
        def _():
            for j, h, target, send in ((left, 0, right, wo_right), (right, 1, left, wo_left)):
                wo_part(me, j, h, wo_core).wait_recv()
                wo_part(target, j, h, send).start()
                wo_part(core, j, h, wo_core).start()

        @pl.when(s == 4)
        def _():
            for j, h in ((left, 1), (right, 0)):
                wo_part(me, j, h, wo_core).wait_recv()
                wo_part(core, j, h, wo_core).start()

        @pl.when(s == 6)
        def _():
            for h in range(2):
                wo_part(me, far, h, wo_core).wait_recv()
                wo_part(core, far, h, wo_core).start()

        here = pl.ds(pl.multiple_of(d * own, own), own)
        out = (mix_s[0:HEAD, here] * (1 / mix_s[HEAD : HEAD + 1, here])).T.astype(jnp.bfloat16)

        @pl.when(s < n - 1)
        def _():
            all_s[stage, :, _ds(s, HEAD)] = out

        @pl.when(s == n - 1)
        def _():
            all_s[o_at(me), :, _ds(s, HEAD)] = out

        pl.when(s > 0)(lambda: result(s - 1).start())

    lax.fori_loop(0, n, last, None)

    for h in range(2):
        wo_own(h).wait()
        for j in (core, at(1, 1), at(chips - 1, 1), at(chips // 2, 1)):
            wo_part(me, j, h, wo_core).wait_recv()
    x_again.wait()
    wide, tall = 512, HEAD
    mine, y_s = o_at(me), left

    def y_copy(t):
        return pltpu.make_async_copy(all_s.at[y_s, :, _ds(t, wide)], y_ref.at[:, _ds(t, wide)], y_sem.at[t])

    def some(a, b):
        for s in range(a, min(b, n - 1)):
            result(s).wait_recv()

        def columns(t, _):
            col = _ds(t, wide)
            wos = [all_s[chip * 2 + s // per, (s % per) * depth : (s % per + 1) * depth, col] for s in range(a, b)]
            w = jnp.concatenate(wos, axis=0)
            for i in range(own // tall):
                rows = slice(i * tall, (i + 1) * tall)
                place = pl.ds(pl.multiple_of(i * width + t * wide, wide), wide)
                part = _dot(all_s[mine, rows, a * HEAD : b * HEAD], w)
                if a:
                    part = part + mix_s[0:tall, place]
                if b < n:
                    mix_s[0:tall, place] = part
                else:
                    all_s[y_s, rows, col] = (all_s[y_s, rows, col].astype(jnp.float32) + part).astype(jnp.bfloat16)
            if b == n:
                y_copy(t).start()

        lax.fori_loop(0, width // wide, columns, None)

    some(0, n // 2)
    some(n // 2, n - 2)
    some(n - 2, n)

    for target in others:
        for m in range(3):
            w_copy(target, m).wait_send()
    for h in range(2):
        wo_first(right, h, wo_right).wait_send()
        wo_first(left, h, wo_left).wait_send()
        wo_first(core, h, wo_core).wait_send()
        for j in (left, right, far):
            wo_part(core, j, h, wo_core).wait_send()
    wo_part(right, left, 0, wo_right).wait_send()
    wo_part(left, right, 1, wo_left).wait_send()
    for s in range(n - 1):
        result(s).wait_send()
    for t in range(width // wide):
        y_copy(t).wait()


def solution(mesh):
    n = mesh.shape["sp"]

    def step(x, gain, wq, wk, wv, wo):
        own, d = x.shape
        tokens, half, low, wide = own * n, HEAD // 2, jnp.bfloat16, jnp.float32
        places = jnp.concatenate([jnp.arange(FINE), FINE * jnp.arange(own // FINE), own * jnp.arange(n)]).astype(wide)
        angle = places[:, None] * THETA ** (-jnp.arange(half, dtype=wide) / half)
        trig = jnp.stack([jnp.cos(angle), jnp.sin(angle)])
        dma = pltpu.SemaphoreType.DMA
        return pl.pallas_call(
            functools.partial(_layer, n),
            name="layer",
            out_shape=jax.ShapeDtypeStruct((own, d), low),
            in_specs=[ANY, VMEM, ANY, ANY, ANY, ANY, VMEM],
            out_specs=ANY,
            scratch_shapes=[
                pltpu.VMEM((n, own, d), low), pltpu.VMEM((3, d, HEAD), low), pltpu.VMEM((own, half), wide), pltpu.VMEM((own, half), wide),
                pltpu.VMEM((HEAD, tokens), low), pltpu.VMEM((tokens, HEAD), low), pltpu.VMEM((HEAD + ONES, tokens), low),
                pltpu.VMEM((1, tokens), wide), pltpu.VMEM((HEAD + ONES, tokens), wide),
                dma, dma((3,)), dma((n, 3)), dma((n, 3)), dma((n, PIECES)), dma((n, PIECES)), dma((n, PIECES)), dma((n, PIECES)),
                pltpu.SemaphoreType.REGULAR, dma((n, 2)), dma((n, 2)), dma((n, 2)), dma((n, 2)), dma((n,)), dma((n,)), dma((d // 512,)),
            ],
            compiler_params=pltpu.CompilerParams(collective_id=0, has_side_effects=True, vmem_limit_bytes=67_043_328),
        )(x, gain.reshape(1, d), wq, wk, wv, wo, trig)

    tokens, whole = P(("dp", "sp"), None), P("sp", None)
    return jax.shard_map(step, mesh=mesh, in_specs=(tokens, P(None), whole, whole, whole, whole), out_specs=tokens, check_vma=False)
```

```python
import functools

import jax
import jax.numpy as jnp
import numpy as np
from jax import lax
from jax.experimental import pallas as pl
from jax.experimental.pallas import tpu as pltpu
from jax.sharding import PartitionSpec as P

HEAD = 256
THETA = 10000
NEG = -1e30
HIDDEN = 2 * NEG
LOG2E = 1.4426950408889634
MESH = pl.DeviceIdType.MESH
ANY = pl.BlockSpec(memory_space=pl.ANY)
VMEM = pl.BlockSpec(memory_space=pltpu.VMEM)
FINE = 32
ONES = 8
PIECES = 4
CUTS = 4
STRIP = 512


def _dot(a, b):
    return jnp.dot(a, b, preferred_element_type=jnp.float32)


def _ds(i, size):
    return pl.ds(pl.multiple_of(i * size, size), size)


def _greet(n, me):
    barrier = pltpu.get_barrier_semaphore()
    for t in range(1, n):
        pl.semaphore_signal(barrier, inc=1, device_id={"sp": (me + t) % n}, device_id_type=MESH)
    pl.semaphore_wait(barrier, n - 1)


def _places(n):
    me = lax.axis_index("sp")
    chips = n // 2
    c, k = me // 2, me % 2
    at = lambda dx, dk=0: ((c + dx) % chips) * 2 + (k + dk) % 2
    return me, at


def _xor(n, a, b):
    out, bit = 0, 1
    while bit < n:
        x, y = (a // bit) % 2, (b // bit) % 2
        out = out + bit * (x + y - 2 * x * y)
        bit *= 2
    return out


def _mask(n, s):
    u, w = s // 2 % 2 * (n // 4) + s // 4, s % 2
    return (1 - w) * (n // 2 + u) + w * (n // 2 - 1 - u)


def _step(n, m):
    far = m // (n // 2)
    u = far * (m - n // 2) + (1 - far) * (n // 2 - 1 - m)
    return u % (n // 4) * 4 + u // (n // 4) * 2 + 1 - far


def _slot(n, s):
    late = s // (n - 3)
    return (1 - late) * s + late * (n - 3 + (s + 4 - n) % 3)


def _layer(n, x_ref, gain_ref, wq_ref, wk_ref, wv_ref, wo_ref, trig_ref, y_ref,
           all_s, w_s, cos_s, sin_s, q_s, k_s, v_s, top_s, mix_s,
           x_sem, own_sem, w_send, w_recv, arrive, to_core, to_right, to_left, ready,
           wo_arrive, wo_core, wo_right, wo_left, o_send, o_recv, y_sem):
    me, at = _places(n)
    own, width = x_ref.shape
    depth = wq_ref.shape[0]
    half = HEAD // 2
    size = own // PIECES
    chips = n // 2
    chip = me // 2
    core, right, left, far = at(0, 1), at(1), at(chips - 1), at(chips // 2)
    mats = (wq_ref, wk_ref, wv_ref)
    others = [at(dx, dk) for dx in (2, 1, 3, 0) for dk in (0, 1) if (dx, dk) != (0, 0)]

    def w_copy(target, m):
        return pltpu.make_async_remote_copy(
            src_ref=mats[m].at[:, _ds(target, HEAD)], dst_ref=w_s.at[m, _ds(me, depth), :],
            send_sem=w_send.at[target, m], recv_sem=w_recv.at[me, m], device_id={"sp": target}, device_id_type=MESH)

    def w_own(m):
        return pltpu.make_async_copy(mats[m].at[:, _ds(me, HEAD)], w_s.at[m, _ds(me, depth), :], own_sem.at[m])

    def w_wait(source, m):
        pltpu.make_async_remote_copy(
            src_ref=mats[m].at[:, _ds(me, HEAD)], dst_ref=w_s.at[m, _ds(source, depth), :],
            send_sem=w_send.at[source, m], recv_sem=w_recv.at[source, m], device_id={"sp": me}, device_id_type=MESH).wait_recv()

    def piece(target, j, p, send):
        ref = all_s.at[j, _ds(p, size), :]
        return pltpu.make_async_remote_copy(src_ref=ref, dst_ref=ref, send_sem=send.at[j, p], recv_sem=arrive.at[j, p],
                                            device_id={"sp": target}, device_id_type=MESH)

    hd = depth // 2
    per = own // depth

    def wo_at(d, j, h):
        s = _slot(n, _step(n, _xor(n, d, j)))
        return all_s.at[d // 2 * 2 + s // per, _ds((s % per) * 2 + h, hd), :]

    def wo_part(target, j, h, send):
        return pltpu.make_async_remote_copy(src_ref=wo_at(me, j, h), dst_ref=wo_at(target, j, h), send_sem=send.at[j, h],
                                            recv_sem=wo_arrive.at[j, h], device_id={"sp": target}, device_id_type=MESH)

    def wo_first(target, h, send):
        return pltpu.make_async_remote_copy(src_ref=wo_ref.at[h * hd : (h + 1) * hd, :], dst_ref=wo_at(target, me, h),
                                            send_sem=send.at[me, h], recv_sem=wo_arrive.at[me, h], device_id={"sp": target}, device_id_type=MESH)

    def wo_own(h):
        return pltpu.make_async_copy(wo_ref.at[h * hd : (h + 1) * hd, :], wo_at(me, me, h), own_sem.at[h])

    def o_at(d):
        return (d // 2 + chips - 1) % chips * 2 + (d + 1) % 2

    stage = at(1, 1)

    def result(s, i):
        d = _xor(n, me, _mask(n, s))
        rows = pl.ds(i * (own // CUTS), own // CUTS)
        return pltpu.make_async_remote_copy(
            src_ref=all_s.at[stage, rows, _ds(s, HEAD)], dst_ref=all_s.at[o_at(d), rows, _ds(_slot(n, s), HEAD)],
            send_sem=o_send.at[s, i], recv_sem=o_recv.at[s, i], device_id={"sp": d}, device_id_type=MESH)

    def project(j, p):
        rows = _ds(p, size)
        place = _ds(j * PIECES + p, size)
        a = all_s[j, rows, :]
        ct, st = trig_ref[0, pl.ds(FINE + own // FINE + j, 1), :], trig_ref[1, pl.ds(FINE + own // FINE + j, 1), :]
        cf, sf = cos_s[rows, :], sin_s[rows, :]
        cos, sin = ct * cf - st * sf, st * cf + ct * sf

        def turned(t):
            t = t.astype(jnp.bfloat16).astype(jnp.float32)
            lo, hi = t[:, :half], t[:, half:]
            return jnp.concatenate([lo * cos - hi * sin, hi * cos + lo * sin], -1)

        q_s[:, place] = turned(_dot(a, w_s[0])).T.astype(jnp.bfloat16)
        k_s[place, :] = turned(_dot(a, w_s[1])).astype(jnp.bfloat16)
        v_s[0:HEAD, place] = _dot(a, w_s[2]).T.astype(jnp.bfloat16)

    e = HEAD**-0.5 * LOG2E
    strips = range(0, own, STRIP)

    def strip(d, at_q):
        return pl.ds(pl.multiple_of(d * own + at_q, STRIP), STRIP)

    def scores(b, count, d, at_q):
        return _dot(k_s[pl.ds(pl.multiple_of(b * own, own), count), :], q_s[:, strip(d, at_q)])

    def values(b, count):
        return v_s[:, pl.ds(pl.multiple_of(b * own, own), count)]

    def itself(d):
        found = []
        for at_q in strips:
            s = scores(d, at_q + STRIP, d, at_q)
            ok = lax.broadcasted_iota(jnp.int32, s.shape, 1) + at_q >= lax.broadcasted_iota(jnp.int32, s.shape, 0)
            found.append(jnp.where(ok, s, HIDDEN))
        weights = []
        for at_q, s in zip(strips, found):
            top = s.max(axis=0, keepdims=True)
            top_s[:, strip(d, at_q)] = top
            weights.append(jnp.exp2((s - top) * e).astype(jnp.bfloat16))
        for at_q, p in zip(strips, weights):
            mix_s[:, strip(d, at_q)] = _dot(values(d, at_q + STRIP), p)

    def earlier(b, d):
        found = [scores(b, own, d, at_q) for at_q in strips]
        weights = []
        for at_q, s in zip(strips, found):
            old = top_s[:, strip(d, at_q)]
            top = jnp.maximum(old, s.max(axis=0, keepdims=True))
            top_s[:, strip(d, at_q)] = top
            weights.append((jnp.exp2((s - top) * e).astype(jnp.bfloat16), jnp.exp2((old - top) * e)))
        for at_q, (p, keep) in zip(strips, weights):
            mix_s[:, strip(d, at_q)] = mix_s[:, strip(d, at_q)] * keep + _dot(values(b, own), p)

    def attend(d, fresh, need):
        if fresh is True:
            itself(d)
        else:
            pl.when(fresh)(lambda: itself(d))

        def one(b, _):
            pl.when(need(b))(lambda: earlier(b, d))

        lax.fori_loop(0, d, one, None)

    _greet(n, me)
    x_copy = pltpu.make_async_copy(x_ref, all_s.at[me], x_sem)
    x_copy.start()
    for target in others:
        for m in range(3):
            w_copy(target, m).start()
    for m in range(3):
        w_own(m).start()
    x_copy.wait()

    def norm(r, _):
        rows = _ds(r, 32)
        wide = all_s[me, rows, :].astype(jnp.float32)
        scale = lax.rsqrt(jnp.mean(wide * wide, -1, keepdims=True) + 1e-6)
        all_s[me, rows, :] = (wide * scale * gain_ref[...].astype(jnp.float32)[None, :]).astype(jnp.bfloat16)

    lax.fori_loop(0, own // 32, norm, None)

    def table(m, _):
        cm, sm = trig_ref[0, pl.ds(FINE + m, 1), :], trig_ref[1, pl.ds(FINE + m, 1), :]
        cf, sf = trig_ref[0, 0:FINE, :], trig_ref[1, 0:FINE, :]
        cos_s[_ds(m, FINE), :] = cm * cf - sm * sf
        sin_s[_ds(m, FINE), :] = sm * cf + cm * sf

    lax.fori_loop(0, own // FINE, table, None)
    v_s[HEAD:, :] = jnp.ones((ONES, v_s.shape[1]), jnp.bfloat16)
    for p in range(PIECES):
        piece(right, me, p, to_right).start()
        piece(left, me, PIECES - 1 - p, to_left).start()
        piece(core, me, p, to_core).start()
    for m in range(3):
        w_own(m).wait()
    for source in others:
        for m in range(3):
            w_wait(source, m)

    def near(t, _):
        other = t // PIECES
        j, p = me + other * (core - me), t % PIECES
        pl.when(other == 1)(lambda: piece(me, j, p, to_core).wait_recv())
        project(j, p)

    lax.fori_loop(0, 2 * PIECES, near, None)
    lax.fori_loop(0, 2, lambda i, _: attend(chip * 2 + i, True, lambda b: b // 2 == chip), None)

    def arrived(j_left, p_left, j_right, p_right, forward):
        for j, p, target, send in ((j_left, p_left, right, to_right), (j_right, p_right, left, to_left)):
            piece(me, j, p, to_core).wait_recv()
            piece(core, j, p, to_core).start()
            if forward is not None:
                pl.when(forward)(lambda: piece(target, j, p, send).start())

    def four(j_left, p_left, j_right, p_right):
        def one(t, _):
            side, other = t % 2, t // 2
            j = j_left + side * (j_right - j_left) + other * (core - me)
            p = p_left + side * (p_right - p_left)
            pl.when(other == 1)(lambda: piece(me, j, p, to_core).wait_recv())
            project(j, p)

        lax.fori_loop(0, 4, one, None)

    def next_chips(p, _):
        arrived(left, p, right, PIECES - 1 - p, p < PIECES // 2)
        four(left, p, right, PIECES - 1 - p)

    lax.fori_loop(0, PIECES, next_chips, None)

    def sent(p, _):
        piece(right, me, p, to_right).wait_send()
        piece(left, me, p, to_left).wait_send()
        for j in (me, left, right):
            piece(core, j, p, to_core).wait_send()

    lax.fori_loop(0, PIECES, sent, None)
    for target in others:
        pl.semaphore_signal(ready, inc=1, device_id={"sp": target}, device_id_type=MESH)
    pl.semaphore_wait(ready, n - 1)
    for h in range(2):
        wo_first(right, h, wo_right).start()
        wo_first(left, 1 - h, wo_left).start()
        wo_first(core, h, wo_core).start()
        wo_own(h).start()

    def middle(i, _):
        t = i // 2
        d = (chip + chips - 1 + t) % chips * 2 + i % 2
        attend(d, t != 1, lambda b: (b // 2 != far // 2) & ((t != 1) | (b // 2 != chip)))

    lax.fori_loop(0, 6, middle, None)

    def far_chip(p, _):
        arrived(far, p, far, PIECES - 1 - p, None)
        four(far, p, far, PIECES - 1 - p)

    lax.fori_loop(0, PIECES // 2, far_chip, None)
    lax.fori_loop(0, PIECES, lambda p, _: piece(core, far, p, to_core).wait_send(), None)

    def passed(p, _):
        piece(right, left, p, to_right).wait_send()
        piece(left, right, PIECES - 1 - p, to_left).wait_send()

    lax.fori_loop(0, PIECES // 2, passed, None)
    x_again = pltpu.make_async_copy(x_ref, all_s.at[left], x_sem)
    x_again.start()

    def last(s, _):
        d = _xor(n, me, _mask(n, s))
        in_far = d // 2 == far // 2
        attend(d, in_far, lambda b: in_far | (b // 2 == far // 2))

        @pl.when(s == 2)
        def _():
            for j, h, target, send in ((left, 0, right, wo_right), (right, 1, left, wo_left)):
                wo_part(me, j, h, wo_core).wait_recv()
                wo_part(target, j, h, send).start()
                wo_part(core, j, h, wo_core).start()

        @pl.when(s == 4)
        def _():
            for j, h in ((left, 1), (right, 0)):
                wo_part(me, j, h, wo_core).wait_recv()
                wo_part(core, j, h, wo_core).start()

        @pl.when(s == 6)
        def _():
            for h in range(2):
                wo_part(me, far, h, wo_core).wait_recv()
                wo_part(core, far, h, wo_core).start()

        here = pl.ds(pl.multiple_of(d * own, own), own)
        out = (mix_s[0:HEAD, here] * (1 / mix_s[HEAD : HEAD + 1, here])).T.astype(jnp.bfloat16)

        @pl.when(s < n - 1)
        def _():
            all_s[stage, :, _ds(s, HEAD)] = out

        @pl.when(s == n - 1)
        def _():
            all_s[o_at(me), :, _ds(_slot(n, s), HEAD)] = out

        @pl.when(s > 0)
        def _():
            for i in range(CUTS):
                result(s - 1, i).start()

    lax.fori_loop(0, n, last, None)

    for h in range(2):
        wo_own(h).wait()
        for j in (core, at(1, 1), at(chips - 1, 1), at(chips // 2, 1)):
            wo_part(me, j, h, wo_core).wait_recv()
    x_again.wait()
    wide, tall = 512, own // CUTS
    mine, y_s = o_at(me), left

    def y_copy(i):
        rows = slice(i * tall, (i + 1) * tall)
        return pltpu.make_async_copy(all_s.at[y_s, rows, :], y_ref.at[rows, :], y_sem.at[i])

    def part(a, b, i, t):
        col, rows = _ds(t, wide), slice(i * tall, (i + 1) * tall)
        place = pl.ds(pl.multiple_of(i * width + t * wide, wide), wide)
        w = jnp.concatenate([all_s[chip * 2 + s // per, (s % per) * depth : (s % per + 1) * depth, col] for s in range(a, b)], axis=0)
        total = _dot(all_s[mine, rows, a * HEAD : b * HEAD], w)
        if a:
            total = total + mix_s[0:tall, place]
        if b < n:
            mix_s[0:tall, place] = total
        else:
            all_s[y_s, rows, col] = (all_s[y_s, rows, col].astype(jnp.float32) + total).astype(jnp.bfloat16)

    def wait_for(steps, cuts):
        for s in steps:
            for i in cuts:
                result(s, i).wait_recv()

    def early(a, b):
        def columns(t, _):
            for i in range(CUTS):
                part(a, b, i, t)

        lax.fori_loop(0, width // wide, columns, None)

    wait_for(range(n // 2), range(CUTS))
    early(0, n // 2)
    wait_for(range(n // 2, n - 3), range(CUTS))
    early(n // 2, n - 2)
    for i in range(CUTS):
        wait_for((n - 3, n - 2), (i,))
        lax.fori_loop(0, width // wide, lambda t, _: part(n - 2, n, i, t), None)
        y_copy(i).start()

    for target in others:
        for m in range(3):
            w_copy(target, m).wait_send()
    for h in range(2):
        wo_first(right, h, wo_right).wait_send()
        wo_first(left, h, wo_left).wait_send()
        wo_first(core, h, wo_core).wait_send()
        for j in (left, right, far):
            wo_part(core, j, h, wo_core).wait_send()
    wo_part(right, left, 0, wo_right).wait_send()
    wo_part(left, right, 1, wo_left).wait_send()
    for i in range(CUTS):
        for s in range(n - 1):
            result(s, i).wait_send()
        y_copy(i).wait()


def solution(mesh):
    n = mesh.shape["sp"]

    def step(x, gain, wq, wk, wv, wo):
        own, d = x.shape
        tokens, half, low, wide = own * n, HEAD // 2, jnp.bfloat16, jnp.float32
        places = np.concatenate([np.arange(FINE), FINE * np.arange(own // FINE), own * np.arange(n)])
        angle = places[:, None] * float(THETA) ** (-np.arange(half) / half)
        trig = jnp.asarray(np.stack([np.cos(angle), np.sin(angle)]), wide)
        dma = pltpu.SemaphoreType.DMA
        return pl.pallas_call(
            functools.partial(_layer, n),
            name="layer",
            out_shape=jax.ShapeDtypeStruct((own, d), low),
            in_specs=[ANY, VMEM, ANY, ANY, ANY, ANY, VMEM],
            out_specs=ANY,
            scratch_shapes=[
                pltpu.VMEM((n, own, d), low), pltpu.VMEM((3, d, HEAD), low), pltpu.VMEM((own, half), wide), pltpu.VMEM((own, half), wide),
                pltpu.VMEM((HEAD, tokens), low), pltpu.VMEM((tokens, HEAD), low), pltpu.VMEM((HEAD + ONES, tokens), low),
                pltpu.VMEM((1, tokens), wide), pltpu.VMEM((HEAD + ONES, tokens), wide),
                dma, dma((3,)), dma((n, 3)), dma((n, 3)), dma((n, PIECES)), dma((n, PIECES)), dma((n, PIECES)), dma((n, PIECES)),
                pltpu.SemaphoreType.REGULAR, dma((n, 2)), dma((n, 2)), dma((n, 2)), dma((n, 2)), dma((n, CUTS)), dma((n, CUTS)), dma((CUTS,)),
            ],
            compiler_params=pltpu.CompilerParams(collective_id=0, has_side_effects=True, vmem_limit_bytes=67_043_328),
        )(x, gain, wq, wk, wv, wo, trig)

    tokens, whole = P(("dp", "sp"), None), P("sp", None)
    return jax.shard_map(step, mesh=mesh, in_specs=(tokens, P(None), whole, whole, whole, whole), out_specs=tokens, check_vma=False)
```

```python
import functools

import jax
import jax.numpy as jnp
import numpy as np
from jax import lax
from jax.experimental import pallas as pl
from jax.experimental.pallas import tpu as pltpu
from jax.sharding import PartitionSpec as P

HEAD = 256
THETA = 10000
NEG = -1e30
HIDDEN = 2 * NEG
LOG2E = 1.4426950408889634
MESH = pl.DeviceIdType.MESH
ANY = pl.BlockSpec(memory_space=pl.ANY)
VMEM = pl.BlockSpec(memory_space=pltpu.VMEM)
FINE = 32
ONES = 8
PIECES = 4
HANDS = 4
CUTS = 4
STRIP = 512


def _dot(a, b):
    return jnp.dot(a, b, preferred_element_type=jnp.float32)


def _ds(i, size):
    return pl.ds(pl.multiple_of(i * size, size), size)


def _greet(n, me):
    barrier = pltpu.get_barrier_semaphore()
    for t in range(1, n):
        pl.semaphore_signal(barrier, inc=1, device_id={"sp": (me + t) % n}, device_id_type=MESH)
    pl.semaphore_wait(barrier, n - 1)


def _places(n):
    me = lax.axis_index("sp")
    chips = n // 2
    c, k = me // 2, me % 2
    at = lambda dx, dk=0: ((c + dx) % chips) * 2 + (k + dk) % 2
    return me, at


def _xor(n, a, b):
    out, bit = 0, 1
    while bit < n:
        x, y = (a // bit) % 2, (b // bit) % 2
        out = out + bit * (x + y - 2 * x * y)
        bit *= 2
    return out


def _mask(n, s):
    u, w = s // 2 % 2 * (n // 4) + s // 4, s % 2
    return (1 - w) * (n // 2 + u) + w * (n // 2 - 1 - u)


def _step(n, m):
    far = m // (n // 2)
    u = far * (m - n // 2) + (1 - far) * (n // 2 - 1 - m)
    return u % (n // 4) * 4 + u // (n // 4) * 2 + 1 - far


def _slot(n, s):
    late = s // (n - 3)
    return (1 - late) * s + late * (n - 3 + (s + 4 - n) % 3)


def _layer(n, x_ref, gain_hbm, wq_ref, wk_ref, wv_ref, wo_ref, trig_hbm, y_ref,
           gain_ref, trig_ref, all_s, w_s, cos_s, sin_s, q_s, k_s, v_s, top_s, mix_s,
           small_sem, x_sem, own_sem, w_send, w_recv, arrive, to_core, to_right, to_left, ready,
           wo_arrive, wo_core, wo_right, wo_left, o_send, o_recv, y_sem):
    me, at = _places(n)
    own, width = x_ref.shape
    depth = wq_ref.shape[0]
    half = HEAD // 2
    size = own // PIECES
    chips = n // 2
    chip = me // 2
    core, right, left, far = at(0, 1), at(1), at(chips - 1), at(chips // 2)
    mats = (wq_ref, wk_ref, wv_ref)
    others = [at(dx, dk) for dx in (2, 1, 3, 0) for dk in (0, 1) if (dx, dk) != (0, 0)]

    def w_copy(target, m):
        return pltpu.make_async_remote_copy(
            src_ref=mats[m].at[:, _ds(target, HEAD)], dst_ref=w_s.at[m, _ds(me, depth), :],
            send_sem=w_send.at[target, m], recv_sem=w_recv.at[me, m], device_id={"sp": target}, device_id_type=MESH)

    def w_own(m):
        return pltpu.make_async_copy(mats[m].at[:, _ds(me, HEAD)], w_s.at[m, _ds(me, depth), :], own_sem.at[m])

    def w_wait(source, m):
        pltpu.make_async_remote_copy(
            src_ref=mats[m].at[:, _ds(me, HEAD)], dst_ref=w_s.at[m, _ds(source, depth), :],
            send_sem=w_send.at[source, m], recv_sem=w_recv.at[source, m], device_id={"sp": me}, device_id_type=MESH).wait_recv()

    def piece(target, j, p, send):
        ref = all_s.at[j, _ds(p, size), :]
        return pltpu.make_async_remote_copy(src_ref=ref, dst_ref=ref, send_sem=send.at[j, p], recv_sem=arrive.at[j, p],
                                            device_id={"sp": target}, device_id_type=MESH)

    hd = depth // 2
    per = own // depth

    def wo_at(d, j, h):
        s = _slot(n, _step(n, _xor(n, d, j)))
        return all_s.at[d // 2 * 2 + s // per, _ds((s % per) * 2 + h, hd), :]

    def wo_part(target, j, h, send):
        return pltpu.make_async_remote_copy(src_ref=wo_at(me, j, h), dst_ref=wo_at(target, j, h), send_sem=send.at[j, h],
                                            recv_sem=wo_arrive.at[j, h], device_id={"sp": target}, device_id_type=MESH)

    def wo_first(target, h, send):
        return pltpu.make_async_remote_copy(src_ref=wo_ref.at[h * hd : (h + 1) * hd, :], dst_ref=wo_at(target, me, h),
                                            send_sem=send.at[me, h], recv_sem=wo_arrive.at[me, h], device_id={"sp": target}, device_id_type=MESH)

    def wo_own(h):
        return pltpu.make_async_copy(wo_ref.at[h * hd : (h + 1) * hd, :], wo_at(me, me, h), own_sem.at[h])

    def o_at(d):
        return (d // 2 + chips - 1) % chips * 2 + (d + 1) % 2

    stage = at(1, 1)

    def result(s, i):
        d = _xor(n, me, _mask(n, s))
        rows = pl.ds(i * (own // CUTS), own // CUTS)
        return pltpu.make_async_remote_copy(
            src_ref=all_s.at[stage, rows, _ds(s, HEAD)], dst_ref=all_s.at[o_at(d), rows, _ds(_slot(n, s), HEAD)],
            send_sem=o_send.at[s, i], recv_sem=o_recv.at[s, i], device_id={"sp": d}, device_id_type=MESH)

    def project(j, p):
        rows = _ds(p, size)
        place = _ds(j * PIECES + p, size)
        a = all_s[j, rows, :]
        ct, st = trig_ref[0, pl.ds(FINE + own // FINE + j, 1), :], trig_ref[1, pl.ds(FINE + own // FINE + j, 1), :]
        cf, sf = cos_s[rows, :], sin_s[rows, :]
        cos, sin = ct * cf - st * sf, st * cf + ct * sf

        def turned(t):
            t = t.astype(jnp.bfloat16).astype(jnp.float32)
            lo, hi = t[:, :half], t[:, half:]
            return jnp.concatenate([lo * cos - hi * sin, hi * cos + lo * sin], -1)

        q_s[:, place] = turned(_dot(a, w_s[0])).T.astype(jnp.bfloat16)
        k_s[place, :] = turned(_dot(a, w_s[1])).astype(jnp.bfloat16)
        v_s[0:HEAD, place] = _dot(a, w_s[2]).T.astype(jnp.bfloat16)

    e = HEAD**-0.5 * LOG2E
    strips = range(0, own, STRIP)

    def strip(d, at_q):
        return pl.ds(pl.multiple_of(d * own + at_q, STRIP), STRIP)

    def scores(b, count, d, at_q):
        return _dot(k_s[pl.ds(pl.multiple_of(b * own, own), count), :], q_s[:, strip(d, at_q)])

    def values(b, count):
        return v_s[:, pl.ds(pl.multiple_of(b * own, own), count)]

    def itself(d):
        found = []
        for at_q in strips:
            s = scores(d, at_q + STRIP, d, at_q)
            ok = lax.broadcasted_iota(jnp.int32, s.shape, 1) + at_q >= lax.broadcasted_iota(jnp.int32, s.shape, 0)
            found.append(jnp.where(ok, s, HIDDEN))
        weights = []
        for at_q, s in zip(strips, found):
            top = s.max(axis=0, keepdims=True)
            top_s[:, strip(d, at_q)] = top
            weights.append(jnp.exp2((s - top) * e).astype(jnp.bfloat16))
        for at_q, p in zip(strips, weights):
            mix_s[:, strip(d, at_q)] = _dot(values(d, at_q + STRIP), p)

    def earlier(b, d):
        found = [scores(b, own, d, at_q) for at_q in strips]
        weights = []
        for at_q, s in zip(strips, found):
            old = top_s[:, strip(d, at_q)]
            top = jnp.maximum(old, s.max(axis=0, keepdims=True))
            top_s[:, strip(d, at_q)] = top
            weights.append((jnp.exp2((s - top) * e).astype(jnp.bfloat16), jnp.exp2((old - top) * e)))
        for at_q, (p, keep) in zip(strips, weights):
            mix_s[:, strip(d, at_q)] = mix_s[:, strip(d, at_q)] * keep + _dot(values(b, own), p)

    def attend(d, fresh, need):
        if fresh is True:
            itself(d)
        else:
            pl.when(fresh)(lambda: itself(d))

        def one(b, _):
            pl.when(need(b))(lambda: earlier(b, d))

        lax.fori_loop(0, d, one, None)

    x_copy = pltpu.make_async_copy(x_ref, all_s.at[me], x_sem)
    small = [pltpu.make_async_copy(gain_hbm, gain_ref, small_sem.at[0]), pltpu.make_async_copy(trig_hbm, trig_ref, small_sem.at[1])]
    _greet(n, me)
    for target in others:
        for m in range(3):
            w_copy(target, m).start()
    x_copy.start()
    for copy in small:
        copy.start()
    for m in range(3):
        w_own(m).start()
    x_copy.wait()
    for copy in small:
        copy.wait()

    def norm(r, _):
        rows = _ds(r, 32)
        wide = all_s[me, rows, :].astype(jnp.float32)
        scale = lax.rsqrt(jnp.mean(wide * wide, -1, keepdims=True) + 1e-6)
        all_s[me, rows, :] = (wide * scale * gain_ref[...].astype(jnp.float32)[None, :]).astype(jnp.bfloat16)

    lax.fori_loop(0, own // 32, norm, None)

    def table(m, _):
        cm, sm = trig_ref[0, pl.ds(FINE + m, 1), :], trig_ref[1, pl.ds(FINE + m, 1), :]
        cf, sf = trig_ref[0, 0:FINE, :], trig_ref[1, 0:FINE, :]
        cos_s[_ds(m, FINE), :] = cm * cf - sm * sf
        sin_s[_ds(m, FINE), :] = sm * cf + cm * sf

    lax.fori_loop(0, own // FINE, table, None)
    v_s[HEAD:, :] = jnp.ones((ONES, v_s.shape[1]), jnp.bfloat16)
    for p in range(PIECES):
        piece(right, me, p, to_right).start()
        piece(left, me, PIECES - 1 - p, to_left).start()
        piece(core, me, p, to_core).start()
    for m in range(3):
        w_own(m).wait()
    for source in others:
        for m in range(3):
            w_wait(source, m)

    def near(t, _):
        other = t // PIECES
        j, p = me + other * (core - me), t % PIECES
        pl.when(other == 1)(lambda: piece(me, j, p, to_core).wait_recv())
        project(j, p)

    lax.fori_loop(0, 2 * PIECES, near, None)
    lax.fori_loop(0, 2, lambda i, _: attend(chip * 2 + i, True, lambda b: b // 2 == chip), None)

    def arrived(j_left, p_left, j_right, p_right, forward):
        for j, p, target, send in ((j_left, p_left, right, to_right), (j_right, p_right, left, to_left)):
            piece(me, j, p, to_core).wait_recv()
            piece(core, j, p, to_core).start()
            if forward is not None:
                pl.when(forward)(lambda: piece(target, j, p, send).start())

    def four(j_left, p_left, j_right, p_right):
        def one(t, _):
            side, other = t % 2, t // 2
            j = j_left + side * (j_right - j_left) + other * (core - me)
            p = p_left + side * (p_right - p_left)
            pl.when(other == 1)(lambda: piece(me, j, p, to_core).wait_recv())
            project(j, p)

        lax.fori_loop(0, 4, one, None)

    def next_chips(p, _):
        arrived(left, p, right, PIECES - 1 - p, p < PIECES // 2)
        four(left, p, right, PIECES - 1 - p)

    lax.fori_loop(0, PIECES, next_chips, None)

    def sent(p, _):
        piece(right, me, p, to_right).wait_send()
        piece(left, me, p, to_left).wait_send()
        for j in (me, left, right):
            piece(core, j, p, to_core).wait_send()

    lax.fori_loop(0, PIECES, sent, None)
    for target in others:
        pl.semaphore_signal(ready, inc=1, device_id={"sp": target}, device_id_type=MESH)
    pl.semaphore_wait(ready, n - 1)
    for h in range(2):
        wo_first(right, h, wo_right).start()
        wo_first(left, 1 - h, wo_left).start()
        wo_first(core, h, wo_core).start()
        wo_own(h).start()

    def middle(i, _):
        t = i // 2
        d = (chip + chips - 1 + t) % chips * 2 + i % 2
        attend(d, t != 1, lambda b: (b // 2 != far // 2) & ((t != 1) | (b // 2 != chip)))

    lax.fori_loop(0, 6, middle, None)

    def far_chip(p, _):
        arrived(far, p, far, PIECES - 1 - p, None)
        four(far, p, far, PIECES - 1 - p)

    lax.fori_loop(0, PIECES // 2, far_chip, None)
    lax.fori_loop(0, PIECES, lambda p, _: piece(core, far, p, to_core).wait_send(), None)

    def passed(p, _):
        piece(right, left, p, to_right).wait_send()
        piece(left, right, PIECES - 1 - p, to_left).wait_send()

    lax.fori_loop(0, PIECES // 2, passed, None)
    x_again = pltpu.make_async_copy(x_ref, all_s.at[left], x_sem)
    x_again.start()

    def last(s, _):
        d = _xor(n, me, _mask(n, s))
        in_far = d // 2 == far // 2
        attend(d, in_far, lambda b: in_far | (b // 2 == far // 2))

        @pl.when(s == 1)
        def _():
            for j, h, target, send in ((left, 0, right, wo_right), (right, 1, left, wo_left)):
                wo_part(me, j, h, wo_core).wait_recv()
                wo_part(target, j, h, send).start()
                wo_part(core, j, h, wo_core).start()

        @pl.when(s == 4)
        def _():
            for j, h in ((left, 1), (right, 0)):
                wo_part(me, j, h, wo_core).wait_recv()
                wo_part(core, j, h, wo_core).start()

        @pl.when(s == 6)
        def _():
            for h in range(2):
                wo_part(me, far, h, wo_core).wait_recv()
                wo_part(core, far, h, wo_core).start()

        here = pl.ds(pl.multiple_of(d * own, own), own)
        out = (mix_s[0:HEAD, here] * (1 / mix_s[HEAD : HEAD + 1, here])).T.astype(jnp.bfloat16)

        @pl.when(s < n - 1)
        def _():
            all_s[stage, :, _ds(s, HEAD)] = out

        @pl.when(s == n - 1)
        def _():
            all_s[o_at(me), :, _ds(_slot(n, s), HEAD)] = out

        @pl.when(s > 0)
        def _():
            for i in range(CUTS):
                result(s - 1, i).start()

    lax.fori_loop(0, n, last, None)

    for h in range(2):
        wo_own(h).wait()
        for j in (core, at(1, 1), at(chips - 1, 1), at(chips // 2, 1)):
            wo_part(me, j, h, wo_core).wait_recv()
    x_again.wait()
    wide, tall = 1024, own // CUTS
    mine, y_s = o_at(me), left

    def y_copy(i):
        rows = slice(i * tall, (i + 1) * tall)
        return pltpu.make_async_copy(all_s.at[y_s, rows, :], y_ref.at[rows, :], y_sem.at[i])

    def part(a, b, r, size, t):
        col, rows = _ds(t, wide), slice(r, r + size)
        sums = slice(r % HEAD, r % HEAD + size), pl.ds(pl.multiple_of(r // HEAD * width + t * wide, wide), wide)
        w = jnp.concatenate([all_s[chip * 2 + s // per, (s % per) * depth : (s % per + 1) * depth, col] for s in range(a, b)], axis=0)
        total = _dot(all_s[mine, rows, a * HEAD : b * HEAD], w)
        if a:
            total = total + mix_s[sums]
        if b < n:
            mix_s[sums] = total
        else:
            all_s[y_s, rows, col] = (all_s[y_s, rows, col].astype(jnp.float32) + total).astype(jnp.bfloat16)

    def wait_for(steps, cuts):
        for s in steps:
            for i in cuts:
                result(s, i).wait_recv()

    def early(a, b):
        def columns(t, _):
            for r in range(0, own, HEAD):
                part(a, b, r, HEAD, t)

        lax.fori_loop(0, width // wide, columns, None)

    wait_for(range(n // 2), range(CUTS))
    early(0, n // 2)
    wait_for(range(n // 2, n - 3), range(CUTS))
    early(n // 2, n - 2)
    for i in range(CUTS):
        wait_for((n - 3, n - 2), (i,))
        lax.fori_loop(0, width // wide, lambda t, _: part(n - 2, n, i * tall, tall, t), None)
        y_copy(i).start()

    for target in others:
        for m in range(3):
            w_copy(target, m).wait_send()
    for h in range(2):
        wo_first(right, h, wo_right).wait_send()
        wo_first(left, h, wo_left).wait_send()
        wo_first(core, h, wo_core).wait_send()
        for j in (left, right, far):
            wo_part(core, j, h, wo_core).wait_send()
    wo_part(right, left, 0, wo_right).wait_send()
    wo_part(left, right, 1, wo_left).wait_send()
    for i in range(CUTS):
        for s in range(n - 1):
            result(s, i).wait_send()
        y_copy(i).wait()


def _hand_on(y_ref, out_ref, part_s, in_sem, out_sem):
    rows = part_s.shape[1]
    parts = part_s.shape[0]
    come = [pltpu.make_async_copy(y_ref.at[i * rows : (i + 1) * rows, :], part_s.at[i], in_sem.at[i]) for i in range(parts)]
    go = [pltpu.make_async_copy(part_s.at[i], out_ref.at[i * rows : (i + 1) * rows, :], out_sem.at[i]) for i in range(parts)]
    for copy in come:
        copy.start()
    for a, b in zip(come, go):
        a.wait()
        b.start()
    for copy in go:
        copy.wait()


def solution(mesh):
    n = mesh.shape["sp"]

    def step(x, gain, wq, wk, wv, wo):
        own, d = x.shape
        tokens, half, low, wide = own * n, HEAD // 2, jnp.bfloat16, jnp.float32
        places = np.concatenate([np.arange(FINE), FINE * np.arange(own // FINE), own * np.arange(n)])
        angle = places[:, None] * float(THETA) ** (-np.arange(half) / half)
        trig = jnp.asarray(np.stack([np.cos(angle), np.sin(angle)]), wide)
        dma = pltpu.SemaphoreType.DMA
        y = pl.pallas_call(
            functools.partial(_layer, n),
            name="layer",
            out_shape=jax.ShapeDtypeStruct((own, d), low),
            in_specs=[ANY] * 7,
            out_specs=ANY,
            scratch_shapes=[
                pltpu.VMEM((d,), low), pltpu.VMEM(trig.shape, wide), pltpu.VMEM((n, own, d), low), pltpu.VMEM((3, d, HEAD), low), pltpu.VMEM((own, half), wide), pltpu.VMEM((own, half), wide),
                pltpu.VMEM((HEAD, tokens), low), pltpu.VMEM((tokens, HEAD), low), pltpu.VMEM((HEAD + ONES, tokens), low),
                pltpu.VMEM((1, tokens), wide), pltpu.VMEM((HEAD + ONES, tokens), wide),
                dma((2,)), dma, dma((3,)), dma((n, 3)), dma((n, 3)), dma((n, PIECES)), dma((n, PIECES)), dma((n, PIECES)), dma((n, PIECES)),
                pltpu.SemaphoreType.REGULAR, dma((n, 2)), dma((n, 2)), dma((n, 2)), dma((n, 2)), dma((n, CUTS)), dma((n, CUTS)), dma((CUTS,)),
            ],
            compiler_params=pltpu.CompilerParams(collective_id=0, has_side_effects=True, vmem_limit_bytes=67_043_328),
        )(x, gain, wq, wk, wv, wo, trig)
        return pl.pallas_call(
            _hand_on,
            name="hand_on",
            out_shape=jax.ShapeDtypeStruct((own, d), low),
            in_specs=[ANY],
            out_specs=ANY,
            scratch_shapes=[pltpu.VMEM((HANDS, own // HANDS, d), low), dma((HANDS,)), dma((HANDS,))],
        )(y)

    tokens, whole = P(("dp", "sp"), None), P("sp", None)
    return jax.shard_map(step, mesh=mesh, in_specs=(tokens, P(None), whole, whole, whole, whole), out_specs=tokens, check_vma=False)
```

```python
import functools

import jax
import jax.numpy as jnp
import numpy as np
from jax import lax
from jax.experimental import pallas as pl
from jax.experimental.pallas import tpu as pltpu
from jax.sharding import PartitionSpec as P

HEAD = 256
THETA = 10000
NEG = -1e30
HIDDEN = 2 * NEG
LOG2E = 1.4426950408889634
MESH = pl.DeviceIdType.MESH
ANY = pl.BlockSpec(memory_space=pl.ANY)
VMEM = pl.BlockSpec(memory_space=pltpu.VMEM)
FINE = 32
ONES = 8
PIECES = 4
HANDS = 4
CUTS = (0, 2, 4, 6, 7, 8)
STRIP = 512


def _dot(a, b):
    return jnp.dot(a, b, preferred_element_type=jnp.float32)


def _ds(i, size):
    return pl.ds(pl.multiple_of(i * size, size), size)


def _greet(n, me):
    barrier = pltpu.get_barrier_semaphore()
    for t in range(1, n):
        pl.semaphore_signal(barrier, inc=1, device_id={"sp": (me + t) % n}, device_id_type=MESH)
    pl.semaphore_wait(barrier, n - 1)


def _places(n):
    me = lax.axis_index("sp")
    chips = n // 2
    c, k = me // 2, me % 2
    at = lambda dx, dk=0: ((c + dx) % chips) * 2 + (k + dk) % 2
    return me, at


def _xor(n, a, b):
    out, bit = 0, 1
    while bit < n:
        x, y = (a // bit) % 2, (b // bit) % 2
        out = out + bit * (x + y - 2 * x * y)
        bit *= 2
    return out


def _mask(n, s):
    u, w = s // 2 % 2 * (n // 4) + s // 4, s % 2
    return (1 - w) * (n // 2 + u) + w * (n // 2 - 1 - u)


def _step(n, m):
    far = m // (n // 2)
    u = far * (m - n // 2) + (1 - far) * (n // 2 - 1 - m)
    return u % (n // 4) * 4 + u // (n // 4) * 2 + 1 - far


def _slot(n, s):
    late = s // (n - 3)
    return (1 - late) * s + late * (n - 3 + (s + 4 - n) % 3)


def _layer(n, x_ref, gain_hbm, wq_ref, wk_ref, wv_ref, wo_ref, trig_hbm, y_ref,
           gain_ref, trig_ref, all_s, w_s, cos_s, sin_s, q_s, k_s, v_s, top_s, mix_s,
           small_sem, x_sem, own_sem, w_send, w_recv, arrive, to_core, to_right, to_left, ready,
           wo_arrive, wo_core, wo_right, wo_left, o_send, o_recv, y_sem):
    me, at = _places(n)
    own, width = x_ref.shape
    depth = wq_ref.shape[0]
    half = HEAD // 2
    size = own // PIECES
    chips = n // 2
    chip = me // 2
    core, right, left, far = at(0, 1), at(1), at(chips - 1), at(chips // 2)
    mats = (wq_ref, wk_ref, wv_ref)
    others = [at(dx, dk) for dx in (2, 1, 3, 0) for dk in (0, 1) if (dx, dk) != (0, 0)]

    def w_copy(target, m):
        return pltpu.make_async_remote_copy(
            src_ref=mats[m].at[:, _ds(target, HEAD)], dst_ref=w_s.at[m, _ds(me, depth), :],
            send_sem=w_send.at[target, m], recv_sem=w_recv.at[me, m], device_id={"sp": target}, device_id_type=MESH)

    def w_own(m):
        return pltpu.make_async_copy(mats[m].at[:, _ds(me, HEAD)], w_s.at[m, _ds(me, depth), :], own_sem.at[m])

    def w_wait(source, m):
        pltpu.make_async_remote_copy(
            src_ref=mats[m].at[:, _ds(me, HEAD)], dst_ref=w_s.at[m, _ds(source, depth), :],
            send_sem=w_send.at[source, m], recv_sem=w_recv.at[source, m], device_id={"sp": me}, device_id_type=MESH).wait_recv()

    def piece(target, j, p, send):
        ref = all_s.at[j, _ds(p, size), :]
        return pltpu.make_async_remote_copy(src_ref=ref, dst_ref=ref, send_sem=send.at[j, p], recv_sem=arrive.at[j, p],
                                            device_id={"sp": target}, device_id_type=MESH)

    hd = depth // 2
    per = own // depth

    def wo_at(d, j, h):
        s = _slot(n, _step(n, _xor(n, d, j)))
        return all_s.at[d // 2 * 2 + s // per, _ds((s % per) * 2 + h, hd), :]

    def wo_part(target, j, h, send):
        return pltpu.make_async_remote_copy(src_ref=wo_at(me, j, h), dst_ref=wo_at(target, j, h), send_sem=send.at[j, h],
                                            recv_sem=wo_arrive.at[j, h], device_id={"sp": target}, device_id_type=MESH)

    def wo_first(target, h, send):
        return pltpu.make_async_remote_copy(src_ref=wo_ref.at[h * hd : (h + 1) * hd, :], dst_ref=wo_at(target, me, h),
                                            send_sem=send.at[me, h], recv_sem=wo_arrive.at[me, h], device_id={"sp": target}, device_id_type=MESH)

    def wo_own(h):
        return pltpu.make_async_copy(wo_ref.at[h * hd : (h + 1) * hd, :], wo_at(me, me, h), own_sem.at[h])

    def o_at(d):
        return (d // 2 + chips - 1) % chips * 2 + (d + 1) % 2

    stage = at(1, 1)

    whole = ((0, own),)
    parts = tuple((a * own // 8, (b - a) * own // 8) for a, b in zip(CUTS, CUTS[1:]))

    def result(s, i, cuts):
        d = _xor(n, me, _mask(n, s))
        rows = pl.ds(*cuts[i])
        return pltpu.make_async_remote_copy(
            src_ref=all_s.at[stage, rows, _ds(s, HEAD)], dst_ref=all_s.at[o_at(d), rows, _ds(_slot(n, s), HEAD)],
            send_sem=o_send.at[s, i], recv_sem=o_recv.at[s, i], device_id={"sp": d}, device_id_type=MESH)

    def project(j, p):
        rows = _ds(p, size)
        place = _ds(j * PIECES + p, size)
        a = all_s[j, rows, :]
        ct, st = trig_ref[0, pl.ds(FINE + own // FINE + j, 1), :], trig_ref[1, pl.ds(FINE + own // FINE + j, 1), :]
        cf, sf = cos_s[rows, :], sin_s[rows, :]
        cos, sin = ct * cf - st * sf, st * cf + ct * sf

        def turned(t):
            t = t.astype(jnp.bfloat16).astype(jnp.float32)
            lo, hi = t[:, :half], t[:, half:]
            return jnp.concatenate([lo * cos - hi * sin, hi * cos + lo * sin], -1)

        q_s[:, place] = turned(_dot(a, w_s[0])).T.astype(jnp.bfloat16)
        k_s[place, :] = turned(_dot(a, w_s[1])).astype(jnp.bfloat16)
        v_s[0:HEAD, place] = _dot(a, w_s[2]).T.astype(jnp.bfloat16)

    e = HEAD**-0.5 * LOG2E
    strips = range(0, own, STRIP)

    def strip(d, at_q):
        return pl.ds(pl.multiple_of(d * own + at_q, STRIP), STRIP)

    def scores(b, count, d, at_q):
        return _dot(k_s[pl.ds(pl.multiple_of(b * own, own), count), :], q_s[:, strip(d, at_q)])

    def values(b, count):
        return v_s[:, pl.ds(pl.multiple_of(b * own, own), count)]

    def itself(d):
        found = []
        for at_q in strips:
            s = scores(d, at_q + STRIP, d, at_q)
            ok = lax.broadcasted_iota(jnp.int32, s.shape, 1) + at_q >= lax.broadcasted_iota(jnp.int32, s.shape, 0)
            found.append(jnp.where(ok, s, HIDDEN))
        weights = []
        for at_q, s in zip(strips, found):
            top = s.max(axis=0, keepdims=True)
            top_s[:, strip(d, at_q)] = top
            weights.append(jnp.exp2((s - top) * e).astype(jnp.bfloat16))
        for at_q, p in zip(strips, weights):
            mix_s[:, strip(d, at_q)] = _dot(values(d, at_q + STRIP), p)

    def earlier(b, d):
        found = [scores(b, own, d, at_q) for at_q in strips]
        weights = []
        for at_q, s in zip(strips, found):
            old = top_s[:, strip(d, at_q)]
            top = jnp.maximum(old, s.max(axis=0, keepdims=True))
            top_s[:, strip(d, at_q)] = top
            weights.append((jnp.exp2((s - top) * e).astype(jnp.bfloat16), jnp.exp2((old - top) * e)))
        for at_q, (p, keep) in zip(strips, weights):
            mix_s[:, strip(d, at_q)] = mix_s[:, strip(d, at_q)] * keep + _dot(values(b, own), p)

    def attend(d, fresh, need):
        if fresh is True:
            itself(d)
        else:
            pl.when(fresh)(lambda: itself(d))

        def one(b, _):
            pl.when(need(b))(lambda: earlier(b, d))

        lax.fori_loop(0, d, one, None)

    x_copy = pltpu.make_async_copy(x_ref, all_s.at[me], x_sem)
    small = [pltpu.make_async_copy(gain_hbm, gain_ref, small_sem.at[0]), pltpu.make_async_copy(trig_hbm, trig_ref, small_sem.at[1])]
    _greet(n, me)
    for target in others:
        for m in range(3):
            w_copy(target, m).start()
    x_copy.start()
    for copy in small:
        copy.start()
    for m in range(3):
        w_own(m).start()
    x_copy.wait()
    for copy in small:
        copy.wait()

    def norm(r, _):
        rows = _ds(r, 32)
        wide = all_s[me, rows, :].astype(jnp.float32)
        scale = lax.rsqrt(jnp.mean(wide * wide, -1, keepdims=True) + 1e-6)
        all_s[me, rows, :] = (wide * scale * gain_ref[...].astype(jnp.float32)[None, :]).astype(jnp.bfloat16)

    lax.fori_loop(0, own // 32, norm, None)

    def table(m, _):
        cm, sm = trig_ref[0, pl.ds(FINE + m, 1), :], trig_ref[1, pl.ds(FINE + m, 1), :]
        cf, sf = trig_ref[0, 0:FINE, :], trig_ref[1, 0:FINE, :]
        cos_s[_ds(m, FINE), :] = cm * cf - sm * sf
        sin_s[_ds(m, FINE), :] = sm * cf + cm * sf

    lax.fori_loop(0, own // FINE, table, None)
    v_s[HEAD:, :] = jnp.ones((ONES, v_s.shape[1]), jnp.bfloat16)
    for p in range(PIECES):
        piece(right, me, p, to_right).start()
        piece(left, me, PIECES - 1 - p, to_left).start()
        piece(core, me, p, to_core).start()
    for m in range(3):
        w_own(m).wait()
    for source in others:
        for m in range(3):
            w_wait(source, m)

    def near(t, _):
        other = t // PIECES
        j, p = me + other * (core - me), t % PIECES
        pl.when(other == 1)(lambda: piece(me, j, p, to_core).wait_recv())
        project(j, p)

    lax.fori_loop(0, 2 * PIECES, near, None)
    lax.fori_loop(0, 2, lambda i, _: attend(chip * 2 + i, True, lambda b: b // 2 == chip), None)

    def arrived(j_left, p_left, j_right, p_right, forward):
        for j, p, target, send in ((j_left, p_left, right, to_right), (j_right, p_right, left, to_left)):
            piece(me, j, p, to_core).wait_recv()
            piece(core, j, p, to_core).start()
            if forward is not None:
                pl.when(forward)(lambda: piece(target, j, p, send).start())

    def four(j_left, p_left, j_right, p_right):
        def one(t, _):
            side, other = t % 2, t // 2
            j = j_left + side * (j_right - j_left) + other * (core - me)
            p = p_left + side * (p_right - p_left)
            pl.when(other == 1)(lambda: piece(me, j, p, to_core).wait_recv())
            project(j, p)

        lax.fori_loop(0, 4, one, None)

    def next_chips(p, _):
        arrived(left, p, right, PIECES - 1 - p, p < PIECES // 2)
        four(left, p, right, PIECES - 1 - p)

    lax.fori_loop(0, PIECES, next_chips, None)

    def sent(p, _):
        piece(right, me, p, to_right).wait_send()
        piece(left, me, p, to_left).wait_send()
        for j in (me, left, right):
            piece(core, j, p, to_core).wait_send()

    lax.fori_loop(0, PIECES, sent, None)
    for target in others:
        pl.semaphore_signal(ready, inc=1, device_id={"sp": target}, device_id_type=MESH)
    pl.semaphore_wait(ready, n - 1)
    for h in range(2):
        wo_first(right, h, wo_right).start()
        wo_first(left, 1 - h, wo_left).start()
        wo_first(core, h, wo_core).start()
        wo_own(h).start()

    def middle(i, _):
        t = i // 2
        d = (chip + chips - 1 + t) % chips * 2 + i % 2
        attend(d, t != 1, lambda b: (b // 2 != far // 2) & ((t != 1) | (b // 2 != chip)))

    lax.fori_loop(0, 6, middle, None)

    def far_chip(p, _):
        arrived(far, p, far, PIECES - 1 - p, None)
        four(far, p, far, PIECES - 1 - p)

    lax.fori_loop(0, PIECES // 2, far_chip, None)
    lax.fori_loop(0, PIECES, lambda p, _: piece(core, far, p, to_core).wait_send(), None)

    def passed(p, _):
        piece(right, left, p, to_right).wait_send()
        piece(left, right, PIECES - 1 - p, to_left).wait_send()

    lax.fori_loop(0, PIECES // 2, passed, None)
    x_again = pltpu.make_async_copy(x_ref, all_s.at[left], x_sem)
    x_again.start()

    def last(s, _):
        d = _xor(n, me, _mask(n, s))
        in_far = d // 2 == far // 2
        attend(d, in_far, lambda b: in_far | (b // 2 == far // 2))

        @pl.when(s == 1)
        def _():
            for j, h, target, send in ((left, 0, right, wo_right), (right, 1, left, wo_left)):
                wo_part(me, j, h, wo_core).wait_recv()
                wo_part(target, j, h, send).start()
                wo_part(core, j, h, wo_core).start()

        @pl.when(s == 4)
        def _():
            for j, h in ((left, 1), (right, 0)):
                wo_part(me, j, h, wo_core).wait_recv()
                wo_part(core, j, h, wo_core).start()

        @pl.when(s == 6)
        def _():
            for h in range(2):
                wo_part(me, far, h, wo_core).wait_recv()
                wo_part(core, far, h, wo_core).start()

        here = pl.ds(pl.multiple_of(d * own, own), own)
        out = (mix_s[0:HEAD, here] * (1 / mix_s[HEAD : HEAD + 1, here])).T.astype(jnp.bfloat16)

        @pl.when(s < n - 1)
        def _():
            all_s[stage, :, _ds(s, HEAD)] = out

        @pl.when(s == n - 1)
        def _():
            all_s[o_at(me), :, _ds(_slot(n, s), HEAD)] = out

        @pl.when((s > 0) & (s < n - 2))
        def _():
            result(s - 1, 0, whole).start()

        @pl.when(s >= n - 2)
        def _():
            for i in range(len(parts)):
                result(s - 1, i, parts).start()

    lax.fori_loop(0, n, last, None)

    for h in range(2):
        wo_own(h).wait()
        for j in (core, at(1, 1), at(chips - 1, 1), at(chips // 2, 1)):
            wo_part(me, j, h, wo_core).wait_recv()
    x_again.wait()
    wide = 1024
    mine, y_s = o_at(me), left

    def y_copy(i):
        rows = pl.ds(*parts[i])
        return pltpu.make_async_copy(all_s.at[y_s, rows, :], y_ref.at[rows, :], y_sem.at[i])

    def part(a, b, r, size, t):
        col, rows = _ds(t, wide), slice(r, r + size)
        sums = slice(r % HEAD, r % HEAD + size), pl.ds(pl.multiple_of(r // HEAD * width + t * wide, wide), wide)
        w = jnp.concatenate([all_s[chip * 2 + s // per, (s % per) * depth : (s % per + 1) * depth, col] for s in range(a, b)], axis=0)
        total = _dot(all_s[mine, rows, a * HEAD : b * HEAD], w)
        if a:
            total = total + mix_s[sums]
        if b < n:
            mix_s[sums] = total
        else:
            all_s[y_s, rows, col] = (all_s[y_s, rows, col].astype(jnp.float32) + total).astype(jnp.bfloat16)

    def early(a, b):
        def columns(t, _):
            for r in range(0, own, HEAD):
                part(a, b, r, HEAD, t)

        lax.fori_loop(0, width // wide, columns, None)

    for s in range(n // 2):
        result(s, 0, whole).wait_recv()
    early(0, n // 2)
    for s in range(n // 2, n - 3):
        result(s, 0, whole).wait_recv()
    early(n // 2, n - 2)
    for i, (r, size) in enumerate(parts):
        for s in (n - 3, n - 2):
            result(s, i, parts).wait_recv()
        lax.fori_loop(0, width // wide, lambda t, _: part(n - 2, n, r, size, t), None)
        y_copy(i).start()

    for target in others:
        for m in range(3):
            w_copy(target, m).wait_send()
    for h in range(2):
        wo_first(right, h, wo_right).wait_send()
        wo_first(left, h, wo_left).wait_send()
        wo_first(core, h, wo_core).wait_send()
        for j in (left, right, far):
            wo_part(core, j, h, wo_core).wait_send()
    wo_part(right, left, 0, wo_right).wait_send()
    wo_part(left, right, 1, wo_left).wait_send()
    for s in range(n - 3):
        result(s, 0, whole).wait_send()
    for i in range(len(parts)):
        for s in (n - 3, n - 2):
            result(s, i, parts).wait_send()
        y_copy(i).wait()


def _hand_on(y_ref, out_ref, part_s, in_sem, out_sem):
    rows = part_s.shape[1]
    parts = part_s.shape[0]
    come = [pltpu.make_async_copy(y_ref.at[i * rows : (i + 1) * rows, :], part_s.at[i], in_sem.at[i]) for i in range(parts)]
    go = [pltpu.make_async_copy(part_s.at[i], out_ref.at[i * rows : (i + 1) * rows, :], out_sem.at[i]) for i in range(parts)]
    for copy in come:
        copy.start()
    for a, b in zip(come, go):
        a.wait()
        b.start()
    for copy in go:
        copy.wait()


def solution(mesh):
    n = mesh.shape["sp"]

    def step(x, gain, wq, wk, wv, wo):
        own, d = x.shape
        tokens, half, low, wide = own * n, HEAD // 2, jnp.bfloat16, jnp.float32
        places = np.concatenate([np.arange(FINE), FINE * np.arange(own // FINE), own * np.arange(n)])
        angle = places[:, None] * float(THETA) ** (-np.arange(half) / half)
        trig = jnp.asarray(np.stack([np.cos(angle), np.sin(angle)]), wide)
        dma = pltpu.SemaphoreType.DMA
        y = pl.pallas_call(
            functools.partial(_layer, n),
            name="layer",
            out_shape=jax.ShapeDtypeStruct((own, d), low),
            in_specs=[ANY] * 7,
            out_specs=ANY,
            scratch_shapes=[
                pltpu.VMEM((d,), low), pltpu.VMEM(trig.shape, wide), pltpu.VMEM((n, own, d), low), pltpu.VMEM((3, d, HEAD), low), pltpu.VMEM((own, half), wide), pltpu.VMEM((own, half), wide),
                pltpu.VMEM((HEAD, tokens), low), pltpu.VMEM((tokens, HEAD), low), pltpu.VMEM((HEAD + ONES, tokens), low),
                pltpu.VMEM((1, tokens), wide), pltpu.VMEM((HEAD + ONES, tokens), wide),
                dma((2,)), dma, dma((3,)), dma((n, 3)), dma((n, 3)), dma((n, PIECES)), dma((n, PIECES)), dma((n, PIECES)), dma((n, PIECES)),
                pltpu.SemaphoreType.REGULAR, dma((n, 2)), dma((n, 2)), dma((n, 2)), dma((n, 2)), dma((n, len(CUTS))), dma((n, len(CUTS))), dma((len(CUTS),)),
            ],
            compiler_params=pltpu.CompilerParams(collective_id=0, has_side_effects=True, vmem_limit_bytes=67_043_328),
        )(x, gain, wq, wk, wv, wo, trig)
        return pl.pallas_call(
            _hand_on,
            name="hand_on",
            out_shape=jax.ShapeDtypeStruct((own, d), low),
            in_specs=[ANY],
            out_specs=ANY,
            scratch_shapes=[pltpu.VMEM((HANDS, own // HANDS, d), low), dma((HANDS,)), dma((HANDS,))],
        )(y)

    tokens, whole = P(("dp", "sp"), None), P("sp", None)
    return jax.shard_map(step, mesh=mesh, in_specs=(tokens, P(None), whole, whole, whole, whole), out_specs=tokens, check_vma=False)
```

```python
import functools

import jax
import jax.numpy as jnp
import numpy as np
from jax import lax
from jax.experimental import pallas as pl
from jax.experimental.pallas import tpu as pltpu
from jax.sharding import PartitionSpec as P

HEAD = 256
THETA = 10000
NEG = -1e30
HIDDEN = 2 * NEG
LOG2E = 1.4426950408889634
MESH = pl.DeviceIdType.MESH
ANY = pl.BlockSpec(memory_space=pl.ANY)
VMEM = pl.BlockSpec(memory_space=pltpu.VMEM)
FINE = 32
ONES = 8
PIECES = 4
HANDS = 4
CUTS = (0, 2, 4, 6, 7, 8)
STRIP = 512


def _dot(a, b):
    return jnp.dot(a, b, preferred_element_type=jnp.float32)


def _ds(i, size):
    return pl.ds(pl.multiple_of(i * size, size), size)


def _greet(n, me):
    barrier = pltpu.get_barrier_semaphore()
    for t in range(1, n):
        pl.semaphore_signal(barrier, inc=1, device_id={"sp": (me + t) % n}, device_id_type=MESH)
    pl.semaphore_wait(barrier, n - 1)


def _places(n):
    me = lax.axis_index("sp")
    chips = n // 2
    c, k = me // 2, me % 2
    at = lambda dx, dk=0: ((c + dx) % chips) * 2 + (k + dk) % 2
    return me, at


def _xor(n, a, b):
    out, bit = 0, 1
    while bit < n:
        x, y = (a // bit) % 2, (b // bit) % 2
        out = out + bit * (x + y - 2 * x * y)
        bit *= 2
    return out


def _mask(n, s):
    u, w = s // 2 % 2 * (n // 4) + s // 4, s % 2
    return (1 - w) * (n // 2 + u) + w * (n // 2 - 1 - u)


def _step(n, m):
    far = m // (n // 2)
    u = far * (m - n // 2) + (1 - far) * (n // 2 - 1 - m)
    return u % (n // 4) * 4 + u // (n // 4) * 2 + 1 - far


def _slot(n, s):
    late = s // (n - 3)
    return (1 - late) * s + late * (n - 3 + (s + 4 - n) % 3)


def _layer(n, x_ref, gain_hbm, wq_ref, wk_ref, wv_ref, wo_ref, trig_hbm, y_ref,
           gain_ref, trig_ref, all_s, w_s, cos_s, sin_s, q_s, k_s, v_s, top_s, mix_s,
           small_sem, x_sem, own_sem, w_send, w_recv, arrive, to_core, to_right, to_left, ready,
           wo_arrive, wo_core, wo_right, wo_left, o_send, o_recv, y_sem):
    me, at = _places(n)
    own, width = x_ref.shape
    depth = wq_ref.shape[0]
    half = HEAD // 2
    size = own // PIECES
    chips = n // 2
    chip = me // 2
    core, right, left, far = at(0, 1), at(1), at(chips - 1), at(chips // 2)
    mats = (wq_ref, wk_ref, wv_ref)
    others = [at(dx, dk) for dx in (2, 1, 3, 0) for dk in (0, 1) if (dx, dk) != (0, 0)]

    def w_copy(target, m):
        return pltpu.make_async_remote_copy(
            src_ref=mats[m].at[:, _ds(target, HEAD)], dst_ref=w_s.at[m, _ds(me, depth), :],
            send_sem=w_send.at[target, m], recv_sem=w_recv.at[me, m], device_id={"sp": target}, device_id_type=MESH)

    def w_own(m):
        return pltpu.make_async_copy(mats[m].at[:, _ds(me, HEAD)], w_s.at[m, _ds(me, depth), :], own_sem.at[m])

    def w_wait(source, m):
        pltpu.make_async_remote_copy(
            src_ref=mats[m].at[:, _ds(me, HEAD)], dst_ref=w_s.at[m, _ds(source, depth), :],
            send_sem=w_send.at[source, m], recv_sem=w_recv.at[source, m], device_id={"sp": me}, device_id_type=MESH).wait_recv()

    def piece(target, j, p, send):
        ref = all_s.at[j, _ds(p, size), :]
        return pltpu.make_async_remote_copy(src_ref=ref, dst_ref=ref, send_sem=send.at[j, p], recv_sem=arrive.at[j, p],
                                            device_id={"sp": target}, device_id_type=MESH)

    hd = depth // 2
    per = own // depth

    def wo_at(d, j, h):
        s = _slot(n, _step(n, _xor(n, d, j)))
        return all_s.at[d // 2 * 2 + s // per, _ds((s % per) * 2 + h, hd), :]

    def wo_part(target, j, h, send):
        return pltpu.make_async_remote_copy(src_ref=wo_at(me, j, h), dst_ref=wo_at(target, j, h), send_sem=send.at[j, h],
                                            recv_sem=wo_arrive.at[j, h], device_id={"sp": target}, device_id_type=MESH)

    def wo_first(target, h, send):
        return pltpu.make_async_remote_copy(src_ref=wo_ref.at[h * hd : (h + 1) * hd, :], dst_ref=wo_at(target, me, h),
                                            send_sem=send.at[me, h], recv_sem=wo_arrive.at[me, h], device_id={"sp": target}, device_id_type=MESH)

    def wo_own(h):
        return pltpu.make_async_copy(wo_ref.at[h * hd : (h + 1) * hd, :], wo_at(me, me, h), own_sem.at[h])

    def o_at(d):
        return (d // 2 + chips - 1) % chips * 2 + (d + 1) % 2

    stage = at(1, 1)

    whole = ((0, own),)
    parts = tuple((a * own // 8, (b - a) * own // 8) for a, b in zip(CUTS, CUTS[1:]))

    def result(s, i, cuts):
        d = _xor(n, me, _mask(n, s))
        rows = pl.ds(*cuts[i])
        return pltpu.make_async_remote_copy(
            src_ref=all_s.at[stage, rows, _ds(s, HEAD)], dst_ref=all_s.at[o_at(d), rows, _ds(_slot(n, s), HEAD)],
            send_sem=o_send.at[s, i], recv_sem=o_recv.at[s, i], device_id={"sp": d}, device_id_type=MESH)

    def project(j, p):
        rows = _ds(p, size)
        place = _ds(j * PIECES + p, size)
        a = all_s[j, rows, :]
        ct, st = trig_ref[0, pl.ds(FINE + own // FINE + j, 1), :], trig_ref[1, pl.ds(FINE + own // FINE + j, 1), :]
        cf, sf = cos_s[rows, :], sin_s[rows, :]
        cos, sin = ct * cf - st * sf, st * cf + ct * sf

        def turned(t):
            t = t.astype(jnp.bfloat16).astype(jnp.float32)
            lo, hi = t[:, :half], t[:, half:]
            return jnp.concatenate([lo * cos - hi * sin, hi * cos + lo * sin], -1)

        q_s[:, place] = turned(_dot(a, w_s[0])).T.astype(jnp.bfloat16)
        k_s[place, :] = turned(_dot(a, w_s[1])).astype(jnp.bfloat16)
        v_s[0:HEAD, place] = _dot(a, w_s[2]).T.astype(jnp.bfloat16)

    e = HEAD**-0.5 * LOG2E
    strips = range(0, own, STRIP)

    def strip(d, at_q):
        return pl.ds(pl.multiple_of(d * own + at_q, STRIP), STRIP)

    def scores(b, count, d, at_q):
        return _dot(k_s[pl.ds(pl.multiple_of(b * own, own), count), :], q_s[:, strip(d, at_q)])

    def values(b, count):
        return v_s[:, pl.ds(pl.multiple_of(b * own, own), count)]

    def itself(d):
        found = []
        for at_q in strips:
            s = scores(d, at_q + STRIP, d, at_q)
            ok = lax.broadcasted_iota(jnp.int32, s.shape, 1) + at_q >= lax.broadcasted_iota(jnp.int32, s.shape, 0)
            found.append(jnp.where(ok, s, HIDDEN))
        weights = []
        for at_q, s in zip(strips, found):
            top = s.max(axis=0, keepdims=True)
            top_s[:, strip(d, at_q)] = top
            weights.append(jnp.exp2((s - top) * e).astype(jnp.bfloat16))
        for at_q, p in zip(strips, weights):
            mix_s[:, strip(d, at_q)] = _dot(values(d, at_q + STRIP), p)

    def earlier(b, d):
        found = [scores(b, own, d, at_q) for at_q in strips]
        weights = []
        for at_q, s in zip(strips, found):
            old = top_s[:, strip(d, at_q)]
            top = jnp.maximum(old, s.max(axis=0, keepdims=True))
            top_s[:, strip(d, at_q)] = top
            weights.append((jnp.exp2((s - top) * e).astype(jnp.bfloat16), jnp.exp2((old - top) * e)))
        for at_q, (p, keep) in zip(strips, weights):
            mix_s[:, strip(d, at_q)] = mix_s[:, strip(d, at_q)] * keep + _dot(values(b, own), p)

    def attend(d, fresh, need):
        if fresh is True:
            itself(d)
        else:
            pl.when(fresh)(lambda: itself(d))

        def one(b, _):
            pl.when(need(b))(lambda: earlier(b, d))

        lax.fori_loop(0, d, one, None)

    x_copy = pltpu.make_async_copy(x_ref, all_s.at[me], x_sem)
    small = [pltpu.make_async_copy(gain_hbm, gain_ref, small_sem.at[0]), pltpu.make_async_copy(trig_hbm, trig_ref, small_sem.at[1])]
    _greet(n, me)
    for m in range(3):
        for target in others:
            w_copy(target, m).start()
    x_copy.start()
    for copy in small:
        copy.start()
    for m in range(3):
        w_own(m).start()
    x_copy.wait()
    for copy in small:
        copy.wait()

    def norm(r, _):
        rows = _ds(r, 32)
        wide = all_s[me, rows, :].astype(jnp.float32)
        scale = lax.rsqrt(jnp.mean(wide * wide, -1, keepdims=True) + 1e-6)
        all_s[me, rows, :] = (wide * scale * gain_ref[...].astype(jnp.float32)[None, :]).astype(jnp.bfloat16)

    lax.fori_loop(0, own // 32, norm, None)

    def table(m, _):
        cm, sm = trig_ref[0, pl.ds(FINE + m, 1), :], trig_ref[1, pl.ds(FINE + m, 1), :]
        cf, sf = trig_ref[0, 0:FINE, :], trig_ref[1, 0:FINE, :]
        cos_s[_ds(m, FINE), :] = cm * cf - sm * sf
        sin_s[_ds(m, FINE), :] = sm * cf + cm * sf

    lax.fori_loop(0, own // FINE, table, None)
    v_s[HEAD:, :] = jnp.ones((ONES, v_s.shape[1]), jnp.bfloat16)
    for p in range(PIECES):
        piece(right, me, p, to_right).start()
        piece(left, me, PIECES - 1 - p, to_left).start()
        piece(core, me, p, to_core).start()
    for m in range(3):
        w_own(m).wait()
    for source in others:
        for m in range(3):
            w_wait(source, m)

    def near(t, _):
        other = t // PIECES
        j, p = me + other * (core - me), t % PIECES
        pl.when(other == 1)(lambda: piece(me, j, p, to_core).wait_recv())
        project(j, p)

    lax.fori_loop(0, 2 * PIECES, near, None)
    lax.fori_loop(0, 2, lambda i, _: attend(chip * 2 + i, True, lambda b: b // 2 == chip), None)

    def arrived(j_left, p_left, j_right, p_right, forward):
        for j, p, target, send in ((j_left, p_left, right, to_right), (j_right, p_right, left, to_left)):
            piece(me, j, p, to_core).wait_recv()
            piece(core, j, p, to_core).start()
            if forward is not None:
                pl.when(forward)(lambda: piece(target, j, p, send).start())

    def four(j_left, p_left, j_right, p_right):
        def one(t, _):
            side, other = t % 2, t // 2
            j = j_left + side * (j_right - j_left) + other * (core - me)
            p = p_left + side * (p_right - p_left)
            pl.when(other == 1)(lambda: piece(me, j, p, to_core).wait_recv())
            project(j, p)

        lax.fori_loop(0, 4, one, None)

    def next_chips(p, _):
        arrived(left, p, right, PIECES - 1 - p, p < PIECES // 2)
        four(left, p, right, PIECES - 1 - p)

    lax.fori_loop(0, PIECES, next_chips, None)

    def sent(p, _):
        piece(right, me, p, to_right).wait_send()
        piece(left, me, p, to_left).wait_send()
        for j in (me, left, right):
            piece(core, j, p, to_core).wait_send()

    lax.fori_loop(0, PIECES, sent, None)
    for target in others:
        pl.semaphore_signal(ready, inc=1, device_id={"sp": target}, device_id_type=MESH)
    pl.semaphore_wait(ready, n - 1)
    for h in range(2):
        wo_first(right, h, wo_right).start()
        wo_first(left, 1 - h, wo_left).start()
        wo_first(core, h, wo_core).start()
        wo_own(h).start()

    def middle(i, _):
        t = i // 2
        d = (chip + chips - 1 + t) % chips * 2 + i % 2
        attend(d, t != 1, lambda b: (b // 2 != far // 2) & ((t != 1) | (b // 2 != chip)))

    lax.fori_loop(0, 6, middle, None)

    def far_chip(p, _):
        arrived(far, p, far, PIECES - 1 - p, None)
        four(far, p, far, PIECES - 1 - p)

    lax.fori_loop(0, PIECES // 2, far_chip, None)
    lax.fori_loop(0, PIECES, lambda p, _: piece(core, far, p, to_core).wait_send(), None)

    def passed(p, _):
        piece(right, left, p, to_right).wait_send()
        piece(left, right, PIECES - 1 - p, to_left).wait_send()

    lax.fori_loop(0, PIECES // 2, passed, None)
    x_again = pltpu.make_async_copy(x_ref, all_s.at[left], x_sem)
    x_again.start()

    def last(s, _):
        d = _xor(n, me, _mask(n, s))
        in_far = d // 2 == far // 2
        attend(d, in_far, lambda b: in_far | (b // 2 == far // 2))

        @pl.when(s == 1)
        def _():
            for j, h, target, send in ((left, 0, right, wo_right), (right, 1, left, wo_left)):
                wo_part(me, j, h, wo_core).wait_recv()
                wo_part(target, j, h, send).start()
                wo_part(core, j, h, wo_core).start()

        @pl.when(s == 4)
        def _():
            for j, h in ((left, 1), (right, 0)):
                wo_part(me, j, h, wo_core).wait_recv()
                wo_part(core, j, h, wo_core).start()

        @pl.when(s == 6)
        def _():
            for h in range(2):
                wo_part(me, far, h, wo_core).wait_recv()
                wo_part(core, far, h, wo_core).start()

        here = pl.ds(pl.multiple_of(d * own, own), own)
        out = (mix_s[0:HEAD, here] * (1 / mix_s[HEAD : HEAD + 1, here])).T.astype(jnp.bfloat16)

        @pl.when(s < n - 1)
        def _():
            all_s[stage, :, _ds(s, HEAD)] = out

        @pl.when(s == n - 1)
        def _():
            all_s[o_at(me), :, _ds(_slot(n, s), HEAD)] = out

        @pl.when((s > 0) & (s < n - 2))
        def _():
            result(s - 1, 0, whole).start()

        @pl.when(s >= n - 2)
        def _():
            for i in range(len(parts)):
                result(s - 1, i, parts).start()

    lax.fori_loop(0, n, last, None)

    for h in range(2):
        wo_own(h).wait()
        for j in (core, at(1, 1), at(chips - 1, 1), at(chips // 2, 1)):
            wo_part(me, j, h, wo_core).wait_recv()
    x_again.wait()
    wide = 1024
    mine, y_s = o_at(me), left

    def y_copy(i):
        rows = pl.ds(*parts[i])
        return pltpu.make_async_copy(all_s.at[y_s, rows, :], y_ref.at[rows, :], y_sem.at[i])

    def part(a, b, r, size, t):
        col, rows = _ds(t, wide), slice(r, r + size)
        sums = slice(r % HEAD, r % HEAD + size), pl.ds(pl.multiple_of(r // HEAD * width + t * wide, wide), wide)
        w = jnp.concatenate([all_s[chip * 2 + s // per, (s % per) * depth : (s % per + 1) * depth, col] for s in range(a, b)], axis=0)
        total = _dot(all_s[mine, rows, a * HEAD : b * HEAD], w)
        if a:
            total = total + mix_s[sums]
        if b < n:
            mix_s[sums] = total
        else:
            all_s[y_s, rows, col] = (all_s[y_s, rows, col].astype(jnp.float32) + total).astype(jnp.bfloat16)

    def early(a, b):
        def columns(t, _):
            for r in range(0, own, HEAD):
                part(a, b, r, HEAD, t)

        lax.fori_loop(0, width // wide, columns, None)

    for s in range(n // 2):
        result(s, 0, whole).wait_recv()
    early(0, n // 2)
    for s in range(n // 2, n - 3):
        result(s, 0, whole).wait_recv()
    early(n // 2, n - 2)
    for i, (r, size) in enumerate(parts):
        for s in (n - 3, n - 2):
            result(s, i, parts).wait_recv()
        lax.fori_loop(0, width // wide, lambda t, _: part(n - 2, n, r, size, t), None)
        y_copy(i).start()

    for target in others:
        for m in range(3):
            w_copy(target, m).wait_send()
    for h in range(2):
        wo_first(right, h, wo_right).wait_send()
        wo_first(left, h, wo_left).wait_send()
        wo_first(core, h, wo_core).wait_send()
        for j in (left, right, far):
            wo_part(core, j, h, wo_core).wait_send()
    wo_part(right, left, 0, wo_right).wait_send()
    wo_part(left, right, 1, wo_left).wait_send()
    for s in range(n - 3):
        result(s, 0, whole).wait_send()
    for i in range(len(parts)):
        for s in (n - 3, n - 2):
            result(s, i, parts).wait_send()
        y_copy(i).wait()


def _hand_on(y_ref, out_ref, part_s, in_sem, out_sem):
    rows = part_s.shape[1]
    parts = part_s.shape[0]
    come = [pltpu.make_async_copy(y_ref.at[i * rows : (i + 1) * rows, :], part_s.at[i], in_sem.at[i]) for i in range(parts)]
    go = [pltpu.make_async_copy(part_s.at[i], out_ref.at[i * rows : (i + 1) * rows, :], out_sem.at[i]) for i in range(parts)]
    for copy in come:
        copy.start()
    for a, b in zip(come, go):
        a.wait()
        b.start()
    for copy in go:
        copy.wait()


def solution(mesh):
    n = mesh.shape["sp"]

    def step(x, gain, wq, wk, wv, wo):
        own, d = x.shape
        tokens, half, low, wide = own * n, HEAD // 2, jnp.bfloat16, jnp.float32
        places = np.concatenate([np.arange(FINE), FINE * np.arange(own // FINE), own * np.arange(n)])
        angle = places[:, None] * float(THETA) ** (-np.arange(half) / half)
        trig = jnp.asarray(np.stack([np.cos(angle), np.sin(angle)]), wide)
        dma = pltpu.SemaphoreType.DMA
        y = pl.pallas_call(
            functools.partial(_layer, n),
            name="layer",
            out_shape=jax.ShapeDtypeStruct((own, d), low),
            in_specs=[ANY] * 7,
            out_specs=ANY,
            scratch_shapes=[
                pltpu.VMEM((d,), low), pltpu.VMEM(trig.shape, wide), pltpu.VMEM((n, own, d), low), pltpu.VMEM((3, d, HEAD), low), pltpu.VMEM((own, half), wide), pltpu.VMEM((own, half), wide),
                pltpu.VMEM((HEAD, tokens), low), pltpu.VMEM((tokens, HEAD), low), pltpu.VMEM((HEAD + ONES, tokens), low),
                pltpu.VMEM((1, tokens), wide), pltpu.VMEM((HEAD + ONES, tokens), wide),
                dma((2,)), dma, dma((3,)), dma((n, 3)), dma((n, 3)), dma((n, PIECES)), dma((n, PIECES)), dma((n, PIECES)), dma((n, PIECES)),
                pltpu.SemaphoreType.REGULAR, dma((n, 2)), dma((n, 2)), dma((n, 2)), dma((n, 2)), dma((n, len(CUTS))), dma((n, len(CUTS))), dma((len(CUTS),)),
            ],
            compiler_params=pltpu.CompilerParams(collective_id=0, has_side_effects=True, vmem_limit_bytes=67_043_328),
        )(x, gain, wq, wk, wv, wo, trig)
        return pl.pallas_call(
            _hand_on,
            name="hand_on",
            out_shape=jax.ShapeDtypeStruct((own, d), low),
            in_specs=[ANY],
            out_specs=ANY,
            scratch_shapes=[pltpu.VMEM((HANDS, own // HANDS, d), low), dma((HANDS,)), dma((HANDS,))],
        )(y)

    tokens, whole = P(("dp", "sp"), None), P("sp", None)
    return jax.shard_map(step, mesh=mesh, in_specs=(tokens, P(None), whole, whole, whole, whole), out_specs=tokens, check_vma=False)
```
